32 devices in a mesh: gx: 4 (over y, x), gy: 8 (over z, core).
Axes of the slice: x: 2, y: 2, z: 4, core: 2. Of those that a mesh axis runs over, the one named last changes fastest.
Arguments:
- matrix_tiles: float32 [8, 32, 6, 128, 128], P('gx', 'gy'), may hold values from -4 to 4.5, as said below
- tile_codes: int32 [8, 32, 6], P('gx', 'gy'), may hold values from 0 to 8, as said below
- tile_counts: int32 [8, 32], P('gx', 'gy'), may hold values from 1 to 6, as said below
- right_side: float32 [8, 32, 128], P('gx', 'gy'), may hold values from -8 to 8
- initial_guess: float32 [8, 32, 128], P('gx', 'gy'), may hold values from -4 to 4
Outputs:
- solution: float32 [8, 32, 128], P('gx', 'gy')
- residual: float32 [8, 32, 128], P('gx', 'gy')
- hessenberg: float32 [5, 4], replicated
The draws below stay inside these ranges and needn't reach their ends.
Inputs may be any that keep to these rules, and one draw needn't show every extreme that they name: tile_codes of slot 0 is 4 (the block itself); the codes of one block row are distinct. `tile_counts`: every block row has at least one live slot; some block row has all 6 slots live. `matrix_tiles`: slot 0 of each block row has a diagonal of 2 to 4 added to its entries.
All inputs are finite; a program needn't handle non-finite values.
Results may differ from the reference program's by a relative error of at most 0.0012.
Values sent between devices are 32-bit elements; how exact they have to be, the bound alone decides.
No kernel may reach another device: no remote copies, remote signals or barrier semaphores. Data moves between devices by JAX's collectives and lax.ppermute only.
A program may use at most 64 MiB of HBM per device.

```python
import jax
import jax.numpy as jnp
from jax import lax

BLK = 128
SLOTS = 6
ITERS = 4
RBX = 2
RBY = 4
BX = 8
BY = 32


def draw_matrix_tiles(key, part):
    first, second = jax.random.split(key, 2)
    shape = (BX, BY, SLOTS, BLK, BLK)
    entries = jax.random.normal(first, shape, jnp.float32)
    tiles = entries * (0.5 / jnp.sqrt(jnp.float32(BLK)))
    diagonal = jax.random.uniform(second, (BX, BY, BLK), jnp.float32, 2.0, 4.0)
    identity = jnp.eye(BLK, dtype=jnp.float32)
    return tiles.at[:, :, 0].add(diagonal[:, :, :, None] * identity)


def draw_tile_codes(key, part):
    scores = jax.random.randint(key, (BX, BY, 8), 0, 1 << 20) * 8 + jnp.arange(8, dtype=jnp.int32)
    ordering = jnp.argsort(scores, axis=-1)
    others = jnp.array([0, 1, 2, 3, 5, 6, 7, 8], jnp.int32)[ordering]
    head = jnp.full((BX, BY, 1), 4, jnp.int32)
    return jnp.concatenate([head, others[:, :, :SLOTS - 1]], axis=-1).astype(jnp.int32)


def draw_tile_counts(key, part):
    first, second, third = jax.random.split(key, 3)
    level = jax.random.randint(first, (BX // RBX, BY // RBY), 2, SLOTS + 1)
    level = jnp.repeat(jnp.repeat(level, RBX, axis=0), RBY, axis=1)
    counts = jnp.minimum(jax.random.randint(second, (BX, BY), 1, SLOTS + 1), level)
    position = jax.random.randint(third, (), 0, BX * BY)
    counts = counts.reshape(-1).at[position].set(SLOTS).reshape(BX, BY)
    return counts.astype(jnp.int32)


def shard_levels(own_key, dims, cuts, low, high):
    def one(dim, shards_of):
        heights = jax.random.uniform(jax.random.fold_in(jax.random.fold_in(own_key, 6), dim), (shards_of,), jnp.float32, low / len(cuts), high / len(cuts))
        return jnp.repeat(jnp.exp(heights), dims[dim] // shards_of).reshape((-1,) + (1,) * (len(dims) - dim - 1))

    factor_of = one(*cuts[0])
    for cut in cuts[1:]:
        factor_of = factor_of * one(*cut)
    return factor_of


def noise(own_key, dims, width, reach, cuts=(), kind=jnp.bfloat16):
    level = shard_levels(own_key, dims, cuts, -0.22, 0.18) if cuts else 1.0
    result = jax.random.normal(own_key, dims, jnp.float32) * width * level
    return jnp.minimum(jnp.maximum(result, -reach), reach).astype(kind)


def setup_inputs(seed: int = 0) -> dict:
    splits = jax.random.split(jax.random.key(seed), 6)
    return {
        "matrix_tiles": draw_matrix_tiles(jax.random.fold_in(splits[5], 71), 0),
        "tile_codes": draw_tile_codes(jax.random.fold_in(splits[5], 71), 0),
        "tile_counts": draw_tile_counts(jax.random.fold_in(splits[5], 71), 0),
        "right_side": noise(splits[3], (BX, BY, BLK), 1.0, 8.0, ((0, 4), (1, 8)), jnp.float32),
        "initial_guess": noise(splits[4], (BX, BY, BLK), 0.5, 4.0, ((0, 4), (1, 8)), jnp.float32),
    }


def nine_blocks(padded, height, breadth):
    return jnp.stack([padded[1 + row_step:1 + row_step + height, 1 + col_step:1 + col_step + breadth] for row_step in (-1, 0, 1) for col_step in (-1, 0, 1)])

def apply_matrix(padded, matrix_tiles, tile_codes, tile_counts):
    height, breadth = (tile_codes.shape[0], tile_codes.shape[1])
    stacked = nine_blocks(padded, height, breadth)
    present = jnp.arange(tile_codes.shape[2], dtype=jnp.int32)[None, None, :] < tile_counts[:, :, None]
    onehot = (tile_codes[:, :, :, None] == jnp.arange(9, dtype=jnp.int32)) & present[:, :, :, None]
    onehot = onehot.astype(jnp.float32)
    picked = jnp.einsum('xysc,cxyk->xysk', onehot, stacked, precision=lax.Precision.HIGHEST)
    return jnp.einsum('xyskl,xysl->xyk', matrix_tiles, picked, precision=lax.Precision.HIGHEST)

def operate(field, matrix_tiles, tile_codes, tile_counts):
    padded = jnp.pad(field, ((1, 1), (1, 1), (0, 0)))
    return apply_matrix(padded, matrix_tiles, tile_codes, tile_counts)

def solve_small(lower, target, steps):
    forward = []
    for row in range(steps):
        total = target[row]
        for column in range(row):
            total = total - lower[row, column] * forward[column]
        forward.append(total / lower[row, row])
    backward = [None] * steps
    for row in reversed(range(steps)):
        total = forward[row]
        for column in range(row + 1, steps):
            total = total - lower[column, row] * backward[column]
        backward[row] = total / lower[row, row]
    return backward

def reference(matrix_tiles, tile_codes, tile_counts, right_side, initial_guess):
    start = right_side - operate(initial_guess, matrix_tiles, tile_codes, tile_counts)
    beta = jnp.sqrt(jnp.sum(start * start))
    basis = [start / beta]
    hessenberg = jnp.zeros((ITERS + 1, ITERS), jnp.float32)
    for column in range(ITERS):
        vector_new = operate(basis[column], matrix_tiles, tile_codes, tile_counts)
        for earlier in range(column + 1):
            inner = jnp.sum(vector_new * basis[earlier])
            hessenberg = hessenberg.at[earlier, column].set(inner)
            vector_new = vector_new - inner * basis[earlier]
        length_new = jnp.sqrt(jnp.sum(vector_new * vector_new))
        hessenberg = hessenberg.at[column + 1, column].set(length_new)
        if column + 1 < ITERS:
            basis.append(vector_new / length_new)
    normal_matrix = jnp.dot(hessenberg.T, hessenberg, precision=lax.Precision.HIGHEST)
    target = beta * hessenberg[0, :]
    lower = jnp.linalg.cholesky(normal_matrix)
    weights = solve_small(lower, target, ITERS)
    solution = initial_guess
    for column in range(ITERS):
        solution = solution + weights[column] * basis[column]
    residual = right_side - operate(solution, matrix_tiles, tile_codes, tile_counts)
    return (solution, residual, hessenberg)
```

```python
import functools

import jax
import jax.numpy as jnp
from jax import lax
from jax.experimental import pallas as pl
from jax.experimental.pallas import tpu as pltpu
from jax.sharding import PartitionSpec as P

ITERS = 4
AXES = ("gx", "gy")
VMEM_BYTES = 12 * 1024 * 1024
OFFSETS = [(dx, dy) for dx in (-1, 0, 1) for dy in (-1, 0, 1) if (dx, dy) != (0, 0)]


class Shape:
    def __init__(self, codes):
        self.rx, self.ry, self.slots = codes.shape
        self.nb = self.rx * self.ry
        self.nx = lax.axis_size("gx")
        self.ny = lax.axis_size("gy")
        self.nd = self.nx * self.ny
        self.rows = max(self.rx, self.ry) + 1
        self.width = self.ry + 2
        self.zero = (self.rx + 2) * (self.ry + 2)

    def edge(self, dx, dy):
        xs = {-1: [0], 0: range(self.rx), 1: [self.rx - 1]}[dx]
        ys = {-1: [0], 0: range(self.ry), 1: [self.ry - 1]}[dy]
        return [(x, y) for x in xs for y in ys]

    def halo(self, dx, dy):
        xs = {-1: [0], 0: range(1, self.rx + 1), 1: [self.rx + 1]}[dx]
        ys = {-1: [0], 0: range(1, self.ry + 1), 1: [self.ry + 1]}[dy]
        return [x * self.width + y for x in xs for y in ys]


def neighbour(shape, ix, iy, dx, dy):
    x, y = ix + dx, iy + dy
    inside = (x >= 0) & (x < shape.nx) & (y >= 0) & (y < shape.ny)
    return jnp.where(inside, x * shape.ny + y, ix * shape.ny + iy)


def pack(shape, here, rows, send):
    for dx, dy in OFFSETS:
        dst = neighbour(shape, here[0], here[1], dx, dy)
        for k, (x, y) in enumerate(shape.edge(dx, dy)):
            send[dst, k] = rows[x * shape.ry + y]


def unpack(shape, here, recv, own, padded):
    for x in range(shape.rx):
        for y in range(shape.ry):
            padded[(x + 1) * shape.width + y + 1] = own[x * shape.ry + y]
    for dx, dy in OFFSETS:
        src = neighbour(shape, here[0], here[1], dx, dy)
        for k, position in enumerate(shape.halo(dx, dy)):
            padded[position] = recv[src, k]
    padded[shape.zero] = jnp.zeros_like(padded[shape.zero])


def matvec(shape, index, tiles, padded):
    blk = tiles.shape[-1]
    eye = lax.broadcasted_iota(jnp.int32, (blk, blk), 0) == lax.broadcasted_iota(
        jnp.int32, (blk, blk), 1
    )
    out = []
    for b in range(shape.nb):
        x, y = divmod(b, shape.ry)
        total = None
        for s in range(shape.slots):
            term = tiles[x, y, s] * padded[index[b, s]]
            total = term if total is None else total + term
        column = jnp.sum(total, axis=1, keepdims=True)
        out.append(jnp.sum(jnp.where(eye, column, 0.0), axis=0, keepdims=True))
    return jnp.concatenate(out, axis=0)


def inner(a, b):
    return jnp.sum(jnp.sum(a * b, axis=1, keepdims=True), axis=0, keepdims=True)


def spread(values):
    lane = lax.broadcasted_iota(jnp.int32, (1, 128), 1)
    row = jnp.zeros((1, 128), jnp.float32)
    for i, value in enumerate(values):
        row = jnp.where(lane == i, value, row)
    return row


def send_dots(shape, row, send):
    for d in range(shape.nd):
        send[d, shape.rows - 1] = row


def sum_dots(shape, recv, at, count):
    parts = [recv[d, at] for d in range(shape.nd)]
    while len(parts) > 1:
        parts = [a + b for a, b in zip(parts[::2], parts[1::2])] + (
            [parts[-1]] if len(parts) % 2 else []
        )
    return [parts[0][:, i : i + 1] for i in range(count)]


def split(value):
    return [value[b : b + 1] for b in range(value.shape[0])]


def first_kernel(shape, here, guess, send):
    rows = [guess[b : b + 1, :] for b in range(shape.nb)]
    pack(shape, here, rows, send)


def start_kernel(shape, here, index, tiles, recv, guess, right, send, start, padded):
    unpack(shape, here, recv, [guess[b : b + 1, :] for b in range(shape.nb)], padded)
    r = right[...] - matvec(shape, index, tiles, padded)
    start[...] = r
    pack(shape, here, split(r), send)
    send_dots(shape, spread([inner(r, r)]), send)


def step_kernel(shape, step, here, index, tiles, recv, *refs):
    keep, (send, v_out, w_out, *h_out, padded) = refs[: 2 * step + 1], refs[2 * step + 1 :]
    last = keep[-1]
    unpack(shape, here, recv, split(last[...]), padded)
    image = matvec(shape, index, tiles, padded)
    sums = sum_dots(shape, recv, shape.rows - 1, step + 1)
    square = sums[step]
    if step == 0:
        length = jnp.sqrt(square)
        scale = 1.0 / length
        v = last[...] * scale
        w = image * scale
        basis = []
    else:
        for i in range(step):
            square = square - sums[i] * sums[i]
        length = jnp.sqrt(square)
        scale = 1.0 / length
        basis = [ref[...] for ref in keep[1 : step + 1]]
        images = [ref[...] for ref in keep[step + 1 :]]
        v = images[-1]
        w = image
        for i in range(step):
            v = v - sums[i] * basis[i]
            w = w - sums[i] * images[i]
        v = v * scale
        w = w * scale
    v_out[...] = v
    w_out[...] = w
    h_out[0][...] = spread(sums[:step] + [length])
    if step + 1 < ITERS:
        pack(shape, here, split(w), send)
    dots = [inner(w, other) for other in basis + [v, w]]
    row = spread(dots)
    if step + 1 < ITERS:
        send_dots(shape, row, send)
    else:
        for d in range(shape.nd):
            send[d, 0] = row


def last_kernel(shape, recv, guess, start, *refs):
    vs, ws, hs, (solution, residual, hess) = (
        refs[:ITERS],
        refs[ITERS : 2 * ITERS],
        refs[2 * ITERS : 3 * ITERS],
        refs[3 * ITERS :],
    )
    sums = sum_dots(shape, recv, 0, ITERS + 1)
    square = sums[ITERS]
    for i in range(ITERS):
        square = square - sums[i] * sums[i]
    columns = []
    beta = hs[0][:, 0:1]
    for j in range(1, ITERS):
        columns.append([hs[j][:, i : i + 1] for i in range(j + 1)])
    columns.append(sums[:ITERS] + [jnp.sqrt(square)])
    hess[...] = jnp.zeros_like(hess)
    row = lax.broadcasted_iota(jnp.int32, hess.shape, 0)
    col = lax.broadcasted_iota(jnp.int32, hess.shape, 1)
    full = jnp.zeros(hess.shape, jnp.float32)
    for j, column in enumerate(columns):
        for i, value in enumerate(column):
            full = jnp.where((row == i) & (col == j), value, full)
    hess[...] = full
    normal = {}
    for a in range(ITERS):
        for b in range(a + 1):
            total = None
            for p, q in zip(columns[a], columns[b]):
                total = p * q if total is None else total + p * q
            normal[a, b] = total
    lower, inverse = {}, {}
    for a in range(ITERS):
        for b in range(a + 1):
            total = normal[a, b]
            for c in range(b):
                total = total - lower[a, c] * lower[b, c]
            if a == b:
                inverse[a] = lax.rsqrt(total)
            else:
                lower[a, b] = total * inverse[b]
    forward = []
    for a in range(ITERS):
        total = beta * columns[a][0]
        for c in range(a):
            total = total - lower[a, c] * forward[c]
        forward.append(total * inverse[a])
    weights = [None] * ITERS
    for a in reversed(range(ITERS)):
        total = forward[a]
        for c in range(a + 1, ITERS):
            total = total - lower[c, a] * weights[c]
        weights[a] = total * inverse[a]
    x = guess[...]
    r = start[...]
    for j in range(ITERS):
        x = x + weights[j] * vs[j][...]
        r = r - weights[j] * ws[j][...]
    solution[...] = x
    residual[...] = r


def table(shape, here, codes, counts):
    x = jnp.arange(shape.rx, dtype=jnp.int32)[:, None, None] + codes // 3
    y = jnp.arange(shape.ry, dtype=jnp.int32)[None, :, None] + codes % 3
    gx = here[0] * shape.rx + x - 1
    gy = here[1] * shape.ry + y - 1
    live = jnp.arange(shape.slots, dtype=jnp.int32) < counts[:, :, None]
    live &= (gx >= 0) & (gx < shape.nx * shape.rx) & (gy >= 0) & (gy < shape.ny * shape.ry)
    return jnp.where(live, x * shape.width + y, shape.zero).reshape(shape.nb, shape.slots)


def body(tiles, codes, counts, right_side, initial_guess):
    shape = Shape(codes)
    blk = tiles.shape[-1]
    here = jnp.stack([lax.axis_index("gx"), lax.axis_index("gy")]).astype(jnp.int32)
    index = table(shape, here, codes, counts)
    flat = (shape.nb, blk)
    guess = initial_guess.reshape(flat)
    right = right_side.reshape(flat)
    smem = pl.BlockSpec(memory_space=pltpu.SMEM)
    vmem = pl.BlockSpec(memory_space=pltpu.VMEM)
    vector = jax.ShapeDtypeStruct(flat, jnp.float32)
    small = jax.ShapeDtypeStruct((1, blk), jnp.float32)
    buffer = jax.ShapeDtypeStruct((shape.nd, shape.rows, 1, blk), jnp.float32)
    params = pltpu.CompilerParams(vmem_limit_bytes=VMEM_BYTES)
    padded = pltpu.VMEM((shape.zero + 1, 1, blk), jnp.float32)

    def exchange(send):
        return lax.all_to_all(send, AXES, 0, 0, tiled=True)

    send = pl.pallas_call(
        functools.partial(first_kernel, shape),
        out_shape=buffer,
        in_specs=[smem, vmem],
        out_specs=vmem,
        compiler_params=params,
        name="first",
    )(here, guess)
    recv = exchange(send)
    send, start = pl.pallas_call(
        functools.partial(start_kernel, shape),
        out_shape=(buffer, vector),
        in_specs=[smem, smem, vmem, vmem, vmem, vmem],
        out_specs=(vmem, vmem),
        scratch_shapes=[padded],
        compiler_params=params,
        name="start",
    )(here, index, tiles, recv, guess, right)
    vs, ws, hs = [], [], []
    for step in range(ITERS):
        recv = exchange(send)
        keep = [start, *vs, *ws]
        final = step + 1 == ITERS
        out = buffer if not final else jax.ShapeDtypeStruct((shape.nd, 1, 1, blk), jnp.float32)
        send, v, w, h = pl.pallas_call(
            functools.partial(step_kernel, shape, step),
            out_shape=(out, vector, vector, small),
            in_specs=[smem, smem] + [vmem] * (2 + len(keep)),
            out_specs=(vmem,) * 4,
            scratch_shapes=[padded],
            compiler_params=params,
            name=f"step{step}",
        )(here, index, tiles, recv, *keep)
        vs.append(v)
        ws.append(w)
        hs.append(h)
    recv = exchange(send)
    solution, residual, hessenberg = pl.pallas_call(
        functools.partial(last_kernel, shape),
        out_shape=(vector, vector, jax.ShapeDtypeStruct((ITERS + 1, ITERS), jnp.float32)),
        in_specs=[vmem] * (3 + 3 * ITERS),
        out_specs=(vmem,) * 3,
        compiler_params=params,
        name="last",
    )(recv, guess, start, *vs, *ws, *hs)
    whole = initial_guess.shape
    return solution.reshape(whole), residual.reshape(whole), hessenberg


def solution(mesh):
    placed = (
        P("gx", "gy", None, None, None),
        P("gx", "gy", None),
        P("gx", "gy"),
        P("gx", "gy", None),
        P("gx", "gy", None),
    )
    return jax.shard_map(
        body,
        mesh=mesh,
        in_specs=placed,
        out_specs=(P("gx", "gy", None), P("gx", "gy", None), P()),
        check_vma=False,
    )
```

```python
import functools

import jax
import jax.numpy as jnp
from jax import lax
from jax.experimental import pallas as pl
from jax.experimental.pallas import tpu as pltpu
from jax.sharding import PartitionSpec as P

ITERS = 4
AXES = ("gx", "gy")
VMEM_BYTES = 12 * 1024 * 1024
OFFSETS = [(dx, dy) for dx in (-1, 0, 1) for dy in (-1, 0, 1) if (dx, dy) != (0, 0)]


class Shape:
    def __init__(self, codes):
        self.rx, self.ry, self.slots = codes.shape
        self.nb = self.rx * self.ry
        self.nx = lax.axis_size("gx")
        self.ny = lax.axis_size("gy")
        self.nd = self.nx * self.ny
        self.rows = max(self.rx, self.ry) + 1
        self.width = self.ry + 2
        self.zero = (self.rx + 2) * (self.ry + 2)
        self.bits = self.zero.bit_length()
        self.fields = 31 // self.bits
        self.words = -(-self.slots // self.fields)

    def edge(self, dx, dy):
        xs = {-1: [0], 0: range(self.rx), 1: [self.rx - 1]}[dx]
        ys = {-1: [0], 0: range(self.ry), 1: [self.ry - 1]}[dy]
        return [(x, y) for x in xs for y in ys]

    def halo(self, dx, dy):
        xs = {-1: [0], 0: range(1, self.rx + 1), 1: [self.rx + 1]}[dx]
        ys = {-1: [0], 0: range(1, self.ry + 1), 1: [self.ry + 1]}[dy]
        return [x * self.width + y for x in xs for y in ys]


def neighbour(shape, dx, dy):
    ix, iy = lax.axis_index("gx"), lax.axis_index("gy")
    x, y = ix + dx, iy + dy
    inside = (x >= 0) & (x < shape.nx) & (y >= 0) & (y < shape.ny)
    return jnp.where(inside, x * shape.ny + y, ix * shape.ny + iy)


def pack(shape, rows, send):
    for dx, dy in OFFSETS:
        dst = neighbour(shape, dx, dy)
        for k, (x, y) in enumerate(shape.edge(dx, dy)):
            send[dst, k] = rows[x * shape.ry + y]


def unpack(shape, recv, own, padded):
    for x in range(shape.rx):
        for y in range(shape.ry):
            padded[(x + 1) * shape.width + y + 1] = own[x * shape.ry + y]
    for dx, dy in OFFSETS:
        src = neighbour(shape, dx, dy)
        for k, position in enumerate(shape.halo(dx, dy)):
            padded[position] = recv[src, k]
    padded[shape.zero] = jnp.zeros_like(padded[shape.zero])


def matvec(shape, index, tiles, padded):
    blk = tiles.shape[-1]
    eye = lax.broadcasted_iota(jnp.int32, (blk, blk), 0) == lax.broadcasted_iota(
        jnp.int32, (blk, blk), 1
    )
    out = []
    words = [[index[b : b + 1, w : w + 1][0, 0] for w in range(shape.words)] for b in range(shape.nb)]
    for b in range(shape.nb):
        x, y = divmod(b, shape.ry)
        total = None
        for s in range(shape.slots):
            word, place = divmod(s, shape.fields)
            row = (words[b][word] >> (place * shape.bits)) & ((1 << shape.bits) - 1)
            term = tiles[x, y, s] * padded[row]
            total = term if total is None else total + term
        column = jnp.sum(total, axis=1, keepdims=True)
        out.append(jnp.sum(jnp.where(eye, column, 0.0), axis=0, keepdims=True))
    return jnp.concatenate(out, axis=0)


def inner(a, b):
    return jnp.sum(jnp.sum(a * b, axis=1, keepdims=True), axis=0, keepdims=True)


def spread(values):
    lane = lax.broadcasted_iota(jnp.int32, (1, 128), 1)
    row = jnp.zeros((1, 128), jnp.float32)
    for i, value in enumerate(values):
        row = jnp.where(lane == i, value, row)
    return row


def send_dots(shape, row, send):
    for d in range(shape.nd):
        send[d, shape.rows - 1] = row


def sum_dots(shape, recv, at, count):
    parts = [recv[d, at] for d in range(shape.nd)]
    while len(parts) > 1:
        parts = [a + b for a, b in zip(parts[::2], parts[1::2])] + (
            [parts[-1]] if len(parts) % 2 else []
        )
    return [parts[0][:, i : i + 1] for i in range(count)]


def split(value):
    return [value[b : b + 1] for b in range(value.shape[0])]


def first_kernel(shape, guess, send):
    rows = [guess[b : b + 1, :] for b in range(shape.nb)]
    pack(shape, rows, send)


def hold_kernel(*refs):
    half = len(refs) // 2
    for source, target in zip(refs[:half], refs[half:]):
        target[...] = source[...]


def start_kernel(shape, index, tiles, recv, guess, right, send, start, padded):
    unpack(shape, recv, [guess[b : b + 1, :] for b in range(shape.nb)], padded)
    r = right[...] - matvec(shape, index, tiles, padded)
    start[...] = r
    pack(shape, split(r), send)
    send_dots(shape, spread([inner(r, r)]), send)


def step_kernel(shape, step, index, tiles, recv, *refs):
    keep, (send, v_out, w_out, *h_out, padded) = refs[: 2 * step + 1], refs[2 * step + 1 :]
    last = keep[-1]
    unpack(shape, recv, split(last[...]), padded)
    image = matvec(shape, index, tiles, padded)
    sums = sum_dots(shape, recv, shape.rows - 1, step + 1)
    square = sums[step]
    if step == 0:
        length = jnp.sqrt(square)
        scale = 1.0 / length
        v = last[...] * scale
        w = image * scale
        basis = []
    else:
        for i in range(step):
            square = square - sums[i] * sums[i]
        length = jnp.sqrt(square)
        scale = 1.0 / length
        basis = [ref[...] for ref in keep[1 : step + 1]]
        images = [ref[...] for ref in keep[step + 1 :]]
        v = images[-1]
        w = image
        for i in range(step):
            v = v - sums[i] * basis[i]
            w = w - sums[i] * images[i]
        v = v * scale
        w = w * scale
    v_out[...] = v
    w_out[...] = w
    h_out[0][...] = spread(sums[:step] + [length])
    if step + 1 < ITERS:
        pack(shape, split(w), send)
    dots = [inner(w, other) for other in basis + [v, w]]
    row = spread(dots)
    if step + 1 < ITERS:
        send_dots(shape, row, send)
    else:
        for d in range(shape.nd):
            send[d, 0] = row


def last_kernel(shape, recv, guess, start, *refs):
    vs, ws, hs, (solution, residual, hess) = (
        refs[:ITERS],
        refs[ITERS : 2 * ITERS],
        refs[2 * ITERS : 3 * ITERS],
        refs[3 * ITERS :],
    )
    sums = sum_dots(shape, recv, 0, ITERS + 1)
    square = sums[ITERS]
    for i in range(ITERS):
        square = square - sums[i] * sums[i]
    columns = []
    beta = hs[0][:, 0:1]
    for j in range(1, ITERS):
        columns.append([hs[j][:, i : i + 1] for i in range(j + 1)])
    columns.append(sums[:ITERS] + [jnp.sqrt(square)])
    row = lax.broadcasted_iota(jnp.int32, hess.shape, 1)
    col = lax.broadcasted_iota(jnp.int32, hess.shape, 0)
    full = jnp.zeros(hess.shape, jnp.float32)
    for j, column in enumerate(columns):
        for i, value in enumerate(column):
            full = jnp.where((row == i) & (col == j), value, full)
    hess[...] = full
    normal = {}
    for a in range(ITERS):
        for b in range(a + 1):
            total = None
            for p, q in zip(columns[a], columns[b]):
                total = p * q if total is None else total + p * q
            normal[a, b] = total
    lower, inverse = {}, {}
    for a in range(ITERS):
        for b in range(a + 1):
            total = normal[a, b]
            for c in range(b):
                total = total - lower[a, c] * lower[b, c]
            if a == b:
                inverse[a] = lax.rsqrt(total)
            else:
                lower[a, b] = total * inverse[b]
    forward = []
    for a in range(ITERS):
        total = beta * columns[a][0]
        for c in range(a):
            total = total - lower[a, c] * forward[c]
        forward.append(total * inverse[a])
    weights = [None] * ITERS
    for a in reversed(range(ITERS)):
        total = forward[a]
        for c in range(a + 1, ITERS):
            total = total - lower[c, a] * weights[c]
        weights[a] = total * inverse[a]
    x = guess[...]
    r = start[...]
    for j in range(ITERS):
        x = x + weights[j] * vs[j][...]
        r = r - weights[j] * ws[j][...]
    solution[...] = x
    residual[...] = r


def table(shape, codes, counts):
    x = jnp.arange(shape.rx, dtype=jnp.int32)[:, None, None] + codes // 3
    y = jnp.arange(shape.ry, dtype=jnp.int32)[None, :, None] + codes % 3
    gx = lax.axis_index("gx") * shape.rx + x - 1
    gy = lax.axis_index("gy") * shape.ry + y - 1
    live = jnp.arange(shape.slots, dtype=jnp.int32) < counts[:, :, None]
    live &= (gx >= 0) & (gx < shape.nx * shape.rx) & (gy >= 0) & (gy < shape.ny * shape.ry)
    place = jnp.where(live, x * shape.width + y, shape.zero).reshape(shape.nb, shape.slots)
    words = [
        sum(place[:, s] << ((s % shape.fields) * shape.bits) for s in range(shape.slots) if s // shape.fields == w)
        for w in range(shape.words)
    ]
    return jnp.stack(words, axis=1)


def body(tiles, codes, counts, right_side, initial_guess):
    shape = Shape(codes)
    blk = tiles.shape[-1]
    index = table(shape, codes, counts)
    flat = (shape.nb, blk)
    guess = initial_guess.reshape(flat)
    right = right_side.reshape(flat)
    vmem = pl.BlockSpec(memory_space=pltpu.VMEM)
    vector = jax.ShapeDtypeStruct(flat, jnp.float32)
    small = jax.ShapeDtypeStruct((1, blk), jnp.float32)
    buffer = jax.ShapeDtypeStruct((shape.nd, shape.rows, 1, blk), jnp.float32)
    params = pltpu.CompilerParams(vmem_limit_bytes=VMEM_BYTES)
    padded = pltpu.VMEM((shape.zero + 1, 1, blk), jnp.float32)

    def exchange(send):
        return lax.all_to_all(send, AXES, 0, 0, tiled=True)

    send = pl.pallas_call(
        functools.partial(first_kernel, shape),
        out_shape=buffer,
        in_specs=[vmem],
        out_specs=vmem,
        compiler_params=params,
        name="first",
    )(guess)
    recv = exchange(send)
    tiles, guess, right = pl.pallas_call(
        hold_kernel,
        out_shape=(jax.ShapeDtypeStruct(tiles.shape, jnp.float32), vector, vector),
        in_specs=[vmem] * 3,
        out_specs=(vmem,) * 3,
        compiler_params=params,
        cost_estimate=pl.CostEstimate(flops=10_000_000, bytes_accessed=0, transcendentals=0),
        name="hold",
    )(tiles, guess, right)
    send, start = pl.pallas_call(
        functools.partial(start_kernel, shape),
        out_shape=(buffer, vector),
        in_specs=[vmem] * 5,
        out_specs=(vmem, vmem),
        scratch_shapes=[padded],
        compiler_params=params,
        name="start",
    )(index, tiles, recv, guess, right)
    vs, ws, hs = [], [], []
    for step in range(ITERS):
        recv = exchange(send)
        keep = [start, *vs, *ws]
        final = step + 1 == ITERS
        out = buffer if not final else jax.ShapeDtypeStruct((shape.nd, 1, 1, blk), jnp.float32)
        send, v, w, h = pl.pallas_call(
            functools.partial(step_kernel, shape, step),
            out_shape=(out, vector, vector, small),
            in_specs=[vmem] * (3 + len(keep)),
            out_specs=(vmem,) * 4,
            scratch_shapes=[padded],
            compiler_params=params,
            name=f"step{step}",
        )(index, tiles, recv, *keep)
        vs.append(v)
        ws.append(w)
        hs.append(h)
    recv = exchange(send)
    solution, residual, hessenberg = pl.pallas_call(
        functools.partial(last_kernel, shape),
        out_shape=(vector, vector, jax.ShapeDtypeStruct((ITERS, ITERS + 1), jnp.float32)),
        in_specs=[vmem] * (3 + 3 * ITERS),
        out_specs=(vmem,) * 3,
        compiler_params=params,
        name="last",
    )(recv, guess, start, *vs, *ws, *hs)
    whole = initial_guess.shape
    return solution.reshape(whole), residual.reshape(whole), hessenberg.T


def solution(mesh):
    placed = (
        P("gx", "gy", None, None, None),
        P("gx", "gy", None),
        P("gx", "gy"),
        P("gx", "gy", None),
        P("gx", "gy", None),
    )
    return jax.shard_map(
        body,
        mesh=mesh,
        in_specs=placed,
        out_specs=(P("gx", "gy", None), P("gx", "gy", None), P()),
        check_vma=False,
    )
```

```python
import functools

import jax
import jax.numpy as jnp
from jax import lax
from jax.experimental import pallas as pl
from jax.experimental.pallas import tpu as pltpu
from jax.sharding import PartitionSpec as P

ITERS = 4
AXES = ("gx", "gy")
VMEM_BYTES = 12 * 1024 * 1024
OFFSETS = [(dx, dy) for dx in (-1, 0, 1) for dy in (-1, 0, 1) if (dx, dy) != (0, 0)]


class Shape:
    def __init__(self, codes):
        self.rx, self.ry, self.slots = codes.shape
        self.nb = self.rx * self.ry
        self.nx = lax.axis_size("gx")
        self.ny = lax.axis_size("gy")
        self.nd = self.nx * self.ny
        self.rows = max(self.rx, self.ry) + 1
        self.width = self.ry + 2
        self.zero = (self.rx + 2) * (self.ry + 2)
        self.bits = self.zero.bit_length()
        self.fields = 24 // self.bits
        self.words = -(-self.slots // self.fields)

    def edge(self, dx, dy):
        xs = {-1: [0], 0: range(self.rx), 1: [self.rx - 1]}[dx]
        ys = {-1: [0], 0: range(self.ry), 1: [self.ry - 1]}[dy]
        return [(x, y) for x in xs for y in ys]

    def halo(self, dx, dy):
        xs = {-1: [0], 0: range(1, self.rx + 1), 1: [self.rx + 1]}[dx]
        ys = {-1: [0], 0: range(1, self.ry + 1), 1: [self.ry + 1]}[dy]
        return [x * self.width + y for x in xs for y in ys]


def neighbour(shape, dx, dy):
    ix, iy = lax.axis_index("gx"), lax.axis_index("gy")
    x, y = ix + dx, iy + dy
    inside = (x >= 0) & (x < shape.nx) & (y >= 0) & (y < shape.ny)
    return jnp.where(inside, x * shape.ny + y, ix * shape.ny + iy)


def pack(shape, rows, send):
    for dx, dy in OFFSETS:
        dst = neighbour(shape, dx, dy)
        for k, (x, y) in enumerate(shape.edge(dx, dy)):
            send[dst, k] = rows[x * shape.ry + y]


def unpack(shape, recv, own, padded):
    for x in range(shape.rx):
        for y in range(shape.ry):
            padded[(x + 1) * shape.width + y + 1] = own[x * shape.ry + y]
    for dx, dy in OFFSETS:
        src = neighbour(shape, dx, dy)
        for k, position in enumerate(shape.halo(dx, dy)):
            padded[position] = recv[src, k]
    padded[shape.zero] = jnp.zeros_like(padded[shape.zero])


def table(shape, codes, counts, index):
    size = (shape.ry, shape.slots)
    slot = lax.broadcasted_iota(jnp.int32, size, 1)
    square = (shape.ry, shape.ry)
    eye = lax.broadcasted_iota(jnp.int32, square, 0) == lax.broadcasted_iota(jnp.int32, square, 1)
    for x in range(shape.rx):
        code = codes[x]
        row = counts[x : x + 1, :].astype(jnp.float32)
        count = jnp.sum(jnp.where(eye, row, 0.0), axis=1, keepdims=True).astype(jnp.int32)
        down = jnp.where(code >= 6, 2, jnp.where(code >= 3, 1, 0))
        px = x + down
        py = lax.broadcasted_iota(jnp.int32, size, 0) + code - 3 * down
        gx = lax.axis_index("gx") * shape.rx + px - 1
        gy = lax.axis_index("gy") * shape.ry + py - 1
        live = slot < count
        live &= (gx >= 0) & (gx < shape.nx * shape.rx) & (gy >= 0) & (gy < shape.ny * shape.ry)
        place = jnp.where(live, px * shape.width + py, shape.zero).astype(jnp.float32)
        for w in range(shape.words):
            word = None
            for s in range(w * shape.fields, min((w + 1) * shape.fields, shape.slots)):
                field = place[:, s : s + 1] * float(1 << ((s % shape.fields) * shape.bits))
                word = field if word is None else word + field
            index[x * shape.ry : (x + 1) * shape.ry, w : w + 1] = word.astype(jnp.int32)


def matvec(shape, index, tiles, padded):
    blk = tiles.shape[-1]
    eye = lax.broadcasted_iota(jnp.int32, (blk, blk), 0) == lax.broadcasted_iota(
        jnp.int32, (blk, blk), 1
    )
    out = []
    words = [[index[b : b + 1, w : w + 1][0, 0] for w in range(shape.words)] for b in range(shape.nb)]
    for b in range(shape.nb):
        x, y = divmod(b, shape.ry)
        total = None
        for s in range(shape.slots):
            word, place = divmod(s, shape.fields)
            row = (words[b][word] >> (place * shape.bits)) & ((1 << shape.bits) - 1)
            term = tiles[x, y, s] * padded[row]
            total = term if total is None else total + term
        column = jnp.sum(total, axis=1, keepdims=True)
        out.append(jnp.sum(jnp.where(eye, column, 0.0), axis=0, keepdims=True))
    return jnp.concatenate(out, axis=0)


def inner(a, b):
    return jnp.sum(jnp.sum(a * b, axis=1, keepdims=True), axis=0, keepdims=True)


def spread(values):
    lane = lax.broadcasted_iota(jnp.int32, (1, 128), 1)
    row = jnp.zeros((1, 128), jnp.float32)
    for i, value in enumerate(values):
        row = jnp.where(lane == i, value, row)
    return row


def send_dots(shape, row, send):
    for d in range(shape.nd):
        send[d, shape.rows - 1] = row


def sum_dots(shape, recv, at, count):
    parts = [recv[d, at] for d in range(shape.nd)]
    while len(parts) > 1:
        parts = [a + b for a, b in zip(parts[::2], parts[1::2])] + (
            [parts[-1]] if len(parts) % 2 else []
        )
    return [parts[0][:, i : i + 1] for i in range(count)]


def split(value):
    return [value[b : b + 1] for b in range(value.shape[0])]


def first_kernel(shape, guess, *refs):
    send = refs[-1]
    rows = [guess[b : b + 1, :] for b in range(shape.nb)]
    pack(shape, rows, send)


def start_kernel(shape, codes, counts, tiles, recv, guess, right, send, start, index, padded):
    table(shape, codes, counts, index)
    unpack(shape, recv, [guess[b : b + 1, :] for b in range(shape.nb)], padded)
    r = right[...] - matvec(shape, index, tiles, padded)
    start[...] = r
    pack(shape, split(r), send)
    send_dots(shape, spread([inner(r, r)]), send)


def step_kernel(shape, step, index, tiles, recv, *refs):
    keep, (send, v_out, w_out, *h_out, padded) = refs[: 2 * step + 1], refs[2 * step + 1 :]
    last = keep[-1]
    unpack(shape, recv, split(last[...]), padded)
    image = matvec(shape, index, tiles, padded)
    sums = sum_dots(shape, recv, shape.rows - 1, step + 1)
    square = sums[step]
    if step == 0:
        length = jnp.sqrt(square)
        scale = 1.0 / length
        v = last[...] * scale
        w = image * scale
        basis = []
    else:
        for i in range(step):
            square = square - sums[i] * sums[i]
        length = jnp.sqrt(square)
        scale = 1.0 / length
        basis = [ref[...] for ref in keep[1 : step + 1]]
        images = [ref[...] for ref in keep[step + 1 :]]
        v = images[-1]
        w = image
        for i in range(step):
            v = v - sums[i] * basis[i]
            w = w - sums[i] * images[i]
        v = v * scale
        w = w * scale
    v_out[...] = v
    w_out[...] = w
    h_out[0][...] = spread(sums[:step] + [length])
    if step + 1 < ITERS:
        pack(shape, split(w), send)
    dots = [inner(w, other) for other in basis + [v, w]]
    row = spread(dots)
    if step + 1 < ITERS:
        send_dots(shape, row, send)
    else:
        for d in range(shape.nd):
            send[d, 0] = row


def last_kernel(shape, recv, guess, start, *refs):
    vs, ws, hs, (solution, residual, hess) = (
        refs[:ITERS],
        refs[ITERS : 2 * ITERS],
        refs[2 * ITERS : 3 * ITERS],
        refs[3 * ITERS :],
    )
    sums = sum_dots(shape, recv, 0, ITERS + 1)
    square = sums[ITERS]
    for i in range(ITERS):
        square = square - sums[i] * sums[i]
    columns = []
    beta = hs[0][:, 0:1]
    for j in range(1, ITERS):
        columns.append([hs[j][:, i : i + 1] for i in range(j + 1)])
    columns.append(sums[:ITERS] + [jnp.sqrt(square)])
    row = lax.broadcasted_iota(jnp.int32, hess.shape, 1)
    col = lax.broadcasted_iota(jnp.int32, hess.shape, 0)
    full = jnp.zeros(hess.shape, jnp.float32)
    for j, column in enumerate(columns):
        for i, value in enumerate(column):
            full = jnp.where((row == i) & (col == j), value, full)
    hess[...] = full
    normal = {}
    for a in range(ITERS):
        for b in range(a + 1):
            total = None
            for p, q in zip(columns[a], columns[b]):
                total = p * q if total is None else total + p * q
            normal[a, b] = total
    lower, inverse = {}, {}
    for a in range(ITERS):
        for b in range(a + 1):
            total = normal[a, b]
            for c in range(b):
                total = total - lower[a, c] * lower[b, c]
            if a == b:
                inverse[a] = lax.rsqrt(total)
            else:
                lower[a, b] = total * inverse[b]
    forward = []
    for a in range(ITERS):
        total = beta * columns[a][0]
        for c in range(a):
            total = total - lower[a, c] * forward[c]
        forward.append(total * inverse[a])
    weights = [None] * ITERS
    for a in reversed(range(ITERS)):
        total = forward[a]
        for c in range(a + 1, ITERS):
            total = total - lower[c, a] * weights[c]
        weights[a] = total * inverse[a]
    x = guess[...]
    r = start[...]
    for j in range(ITERS):
        x = x + weights[j] * vs[j][...]
        r = r - weights[j] * ws[j][...]
    solution[...] = x
    residual[...] = r


def body(tiles, codes, counts, right_side, initial_guess):
    shape = Shape(codes)
    blk = tiles.shape[-1]
    flat = (shape.nb, blk)
    guess = initial_guess.reshape(flat)
    right = right_side.reshape(flat)
    vmem = pl.BlockSpec(memory_space=pltpu.VMEM)
    vector = jax.ShapeDtypeStruct(flat, jnp.float32)
    small = jax.ShapeDtypeStruct((1, blk), jnp.float32)
    buffer = jax.ShapeDtypeStruct((shape.nd, shape.rows, 1, blk), jnp.float32)
    params = pltpu.CompilerParams(vmem_limit_bytes=VMEM_BYTES)
    padded = pltpu.VMEM((shape.zero + 1, 1, blk), jnp.float32)

    def exchange(send):
        return lax.all_to_all(send, AXES, 0, 0, tiled=True)

    send = pl.pallas_call(
        functools.partial(first_kernel, shape),
        out_shape=jax.ShapeDtypeStruct((shape.nd, shape.rows - 1, 1, blk), jnp.float32),
        in_specs=[vmem] + [pl.BlockSpec(memory_space=pltpu.HBM)] * 4,
        out_specs=vmem,
        compiler_params=params,
        name="first",
    )(guess, *(pltpu.with_memory_space_constraint(x, pltpu.HBM) for x in (tiles, right, codes, counts)))
    recv = exchange(send)
    send, start, index = pl.pallas_call(
        functools.partial(start_kernel, shape),
        out_shape=(buffer, vector, jax.ShapeDtypeStruct((shape.nb, shape.words), jnp.int32)),
        in_specs=[vmem] * 6,
        out_specs=(vmem,) * 3,
        scratch_shapes=[padded],
        compiler_params=params,
        name="start",
    )(codes, counts, tiles, recv, guess, right)
    vs, ws, hs = [], [], []
    for step in range(ITERS):
        recv = exchange(send)
        keep = [start, *vs, *ws]
        final = step + 1 == ITERS
        out = buffer if not final else jax.ShapeDtypeStruct((shape.nd, 1, 1, blk), jnp.float32)
        send, v, w, h = pl.pallas_call(
            functools.partial(step_kernel, shape, step),
            out_shape=(out, vector, vector, small),
            in_specs=[vmem] * (3 + len(keep)),
            out_specs=(vmem,) * 4,
            scratch_shapes=[padded],
            compiler_params=params,
            name=f"step{step}",
        )(index, tiles, recv, *keep)
        vs.append(v)
        ws.append(w)
        hs.append(h)
    recv = exchange(send)
    solution, residual, hessenberg = pl.pallas_call(
        functools.partial(last_kernel, shape),
        out_shape=(vector, vector, jax.ShapeDtypeStruct((ITERS, ITERS + 1), jnp.float32)),
        in_specs=[vmem] * (3 + 3 * ITERS),
        out_specs=(vmem,) * 3,
        compiler_params=params,
        name="last",
    )(recv, guess, start, *vs, *ws, *hs)
    whole = initial_guess.shape
    return solution.reshape(whole), residual.reshape(whole), hessenberg.T


def solution(mesh):
    placed = (
        P("gx", "gy", None, None, None),
        P("gx", "gy", None),
        P("gx", "gy"),
        P("gx", "gy", None),
        P("gx", "gy", None),
    )
    return jax.shard_map(
        body,
        mesh=mesh,
        in_specs=placed,
        out_specs=(P("gx", "gy", None), P("gx", "gy", None), P()),
        check_vma=False,
    )
```

```python
import functools

import jax
import jax.numpy as jnp
from jax import lax
from jax.experimental import pallas as pl
from jax.experimental.pallas import tpu as pltpu
from jax.sharding import PartitionSpec as P

ITERS = 4
AXES = ("gx", "gy")
VMEM_BYTES = 12 * 1024 * 1024
OFFSETS = [(dx, dy) for dx in (-1, 0, 1) for dy in (-1, 0, 1) if (dx, dy) != (0, 0)]


class Shape:
    def __init__(self, codes):
        self.rx, self.ry, self.slots = codes.shape
        self.nb = self.rx * self.ry
        self.nx = lax.axis_size("gx")
        self.ny = lax.axis_size("gy")
        self.nd = self.nx * self.ny
        self.rows = max(self.rx, self.ry) + 1
        self.width = self.ry + 2
        self.zero = (self.rx + 2) * (self.ry + 2)
        self.bits = self.zero.bit_length()
        self.fields = 31 // self.bits
        self.words = -(-self.slots // self.fields)

    def edge(self, dx, dy):
        xs = {-1: [0], 0: range(self.rx), 1: [self.rx - 1]}[dx]
        ys = {-1: [0], 0: range(self.ry), 1: [self.ry - 1]}[dy]
        return [(x, y) for x in xs for y in ys]

    def halo(self, dx, dy):
        xs = {-1: [0], 0: range(1, self.rx + 1), 1: [self.rx + 1]}[dx]
        ys = {-1: [0], 0: range(1, self.ry + 1), 1: [self.ry + 1]}[dy]
        return [x * self.width + y for x in xs for y in ys]


def neighbour(shape, dx, dy):
    ix, iy = lax.axis_index("gx"), lax.axis_index("gy")
    x, y = ix + dx, iy + dy
    inside = (x >= 0) & (x < shape.nx) & (y >= 0) & (y < shape.ny)
    return jnp.where(inside, x * shape.ny + y, ix * shape.ny + iy)


def pack(shape, rows, send):
    for dx, dy in OFFSETS:
        dst = neighbour(shape, dx, dy)
        for k, (x, y) in enumerate(shape.edge(dx, dy)):
            send[dst, k] = rows[x * shape.ry + y]


def unpack(shape, recv, own, padded):
    for x in range(shape.rx):
        for y in range(shape.ry):
            padded[(x + 1) * shape.width + y + 1] = own[x * shape.ry + y]
    for dx, dy in OFFSETS:
        src = neighbour(shape, dx, dy)
        for k, position in enumerate(shape.halo(dx, dy)):
            padded[position] = recv[src, k]
    padded[shape.zero] = jnp.zeros_like(padded[shape.zero])


def table(shape, codes, counts, index):
    size = (shape.ry, shape.slots)
    slot = lax.broadcasted_iota(jnp.int32, size, 1)
    square = (shape.ry, shape.ry)
    eye = lax.broadcasted_iota(jnp.int32, square, 0) == lax.broadcasted_iota(jnp.int32, square, 1)
    for x in range(shape.rx):
        code = codes[x]
        row = counts[x : x + 1, :].astype(jnp.float32)
        count = jnp.sum(jnp.where(eye, row, 0.0), axis=1, keepdims=True).astype(jnp.int32)
        down = jnp.where(code >= 6, 2, jnp.where(code >= 3, 1, 0))
        px = x + down
        py = lax.broadcasted_iota(jnp.int32, size, 0) + code - 3 * down
        gx = lax.axis_index("gx") * shape.rx + px - 1
        gy = lax.axis_index("gy") * shape.ry + py - 1
        live = slot < count
        live &= (gx >= 0) & (gx < shape.nx * shape.rx) & (gy >= 0) & (gy < shape.ny * shape.ry)
        place = jnp.where(live, px * shape.width + py, shape.zero)
        place = place << (lax.rem(slot, shape.fields) * shape.bits)
        for w in range(shape.words):
            word = None
            for s in range(w * shape.fields, min((w + 1) * shape.fields, shape.slots)):
                field = place[:, s : s + 1]
                word = field if word is None else word | field
            index[x * shape.ry : (x + 1) * shape.ry, w : w + 1] = word


def matvec(shape, index, tiles, padded):
    blk = tiles.shape[-1]
    eye = lax.broadcasted_iota(jnp.int32, (blk, blk), 0) == lax.broadcasted_iota(
        jnp.int32, (blk, blk), 1
    )
    out = []
    words = [[index[b : b + 1, w : w + 1][0, 0] for w in range(shape.words)] for b in range(shape.nb)]
    for b in range(shape.nb):
        x, y = divmod(b, shape.ry)
        total = None
        for s in range(shape.slots):
            word, place = divmod(s, shape.fields)
            row = (words[b][word] >> (place * shape.bits)) & ((1 << shape.bits) - 1)
            term = tiles[x, y, s] * padded[row]
            total = term if total is None else total + term
        column = jnp.sum(total, axis=1, keepdims=True)
        row = jnp.zeros((8, blk), jnp.float32)
        for k in range(0, blk, 8):
            row = jnp.where(eye[k : k + 8], column[k : k + 8], row)
        out.append(jnp.sum(row, axis=0, keepdims=True))
    return jnp.concatenate(out, axis=0)


def inner(a, b):
    return jnp.sum(jnp.sum(a * b, axis=1, keepdims=True), axis=0, keepdims=True)


def spread(values):
    lane = lax.broadcasted_iota(jnp.int32, (1, 128), 1)
    row = jnp.zeros((1, 128), jnp.float32)
    for i, value in enumerate(values):
        row = jnp.where(lane == i, value, row)
    return row


def send_dots(shape, row, send):
    for d in range(shape.nd):
        send[d, shape.rows - 1] = row


def sum_dots(shape, recv, at, count):
    parts = [recv[d, at] for d in range(shape.nd)]
    while len(parts) > 1:
        parts = [a + b for a, b in zip(parts[::2], parts[1::2])] + (
            [parts[-1]] if len(parts) % 2 else []
        )
    return [parts[0][:, i : i + 1] for i in range(count)]


def split(value):
    return [value[b : b + 1] for b in range(value.shape[0])]


def first_kernel(shape, guess, *refs):
    send = refs[-1]
    rows = [guess[b : b + 1, :] for b in range(shape.nb)]
    pack(shape, rows, send)


def start_kernel(shape, codes, counts, tiles, recv, guess, right, send, start, index, padded):
    table(shape, codes, counts, index)
    unpack(shape, recv, [guess[b : b + 1, :] for b in range(shape.nb)], padded)
    r = right[...] - matvec(shape, index, tiles, padded)
    start[...] = r
    pack(shape, split(r), send)


def first_step_kernel(shape, index, tiles, recv, start, send, image, padded):
    r = start[...]
    unpack(shape, recv, split(r), padded)
    t = matvec(shape, index, tiles, padded)
    image[...] = t
    pack(shape, split(t), send)
    send_dots(shape, spread([inner(r, r), inner(t, r), inner(t, t)]), send)


def step_kernel(shape, step, index, tiles, recv, *refs):
    count = 2 * step
    keep, outs = refs[:count], list(refs[count:])
    padded = outs.pop()
    last = keep[-1][...]
    unpack(shape, recv, split(last), padded)
    image = matvec(shape, index, tiles, padded)
    if step == 1:
        whole, cross, square = sum_dots(shape, recv, shape.rows - 1, 3)
        beta = jnp.sqrt(whole)
        inverse = 1.0 / beta
        sums = [cross / whole]
        square = square / whole
        basis = [keep[0][...] * inverse]
        images = [last * inverse]
        image = image * inverse
    else:
        *sums, square = sum_dots(shape, recv, shape.rows - 1, step + 1)
        basis = [ref[...] for ref in keep[:step]]
        images = [ref[...] for ref in keep[step:]]
    for value in sums:
        square = square - value * value
    length = jnp.sqrt(square)
    scale = 1.0 / length
    v, w = images[-1], image
    for value, b, a in zip(sums, basis, images):
        v = v - value * b
        w = w - value * a
    v = v * scale
    w = w * scale
    if step + 1 < ITERS:
        pack(shape, split(w), outs[0])
    row = spread([inner(w, other) for other in basis + [v, w]])
    if step + 1 < ITERS:
        send_dots(shape, row, outs[0])
    else:
        for d in range(shape.nd):
            outs[0][d, 0] = row
    outs[1][...] = v
    outs[2][...] = w
    outs[3][...] = spread(sums + [length])
    if step == 1:
        outs[4][...] = basis[0]
        outs[5][...] = images[0]
        outs[6][...] = spread([beta])


def last_kernel(shape, recv, guess, start, *refs):
    vs, ws, hs, (solution, residual, hess) = (
        refs[:ITERS],
        refs[ITERS : 2 * ITERS],
        refs[2 * ITERS : 3 * ITERS],
        refs[3 * ITERS :],
    )
    sums = sum_dots(shape, recv, 0, ITERS + 1)
    square = sums[ITERS]
    for i in range(ITERS):
        square = square - sums[i] * sums[i]
    columns = []
    beta = hs[0][:, 0:1]
    for j in range(1, ITERS):
        columns.append([hs[j][:, i : i + 1] for i in range(j + 1)])
    columns.append(sums[:ITERS] + [jnp.sqrt(square)])
    row = lax.broadcasted_iota(jnp.int32, hess.shape, 1)
    col = lax.broadcasted_iota(jnp.int32, hess.shape, 0)
    full = jnp.zeros(hess.shape, jnp.float32)
    for j, column in enumerate(columns):
        for i, value in enumerate(column):
            full = jnp.where((row == i) & (col == j), value, full)
    hess[...] = full
    normal = {}
    for a in range(ITERS):
        for b in range(a + 1):
            total = None
            for p, q in zip(columns[a], columns[b]):
                total = p * q if total is None else total + p * q
            normal[a, b] = total
    lower, inverse = {}, {}
    for a in range(ITERS):
        for b in range(a + 1):
            total = normal[a, b]
            for c in range(b):
                total = total - lower[a, c] * lower[b, c]
            if a == b:
                inverse[a] = lax.rsqrt(total)
            else:
                lower[a, b] = total * inverse[b]
    forward = []
    for a in range(ITERS):
        total = beta * columns[a][0]
        for c in range(a):
            total = total - lower[a, c] * forward[c]
        forward.append(total * inverse[a])
    weights = [None] * ITERS
    for a in reversed(range(ITERS)):
        total = forward[a]
        for c in range(a + 1, ITERS):
            total = total - lower[c, a] * weights[c]
        weights[a] = total * inverse[a]
    x = guess[...]
    r = start[...]
    for j in range(ITERS):
        x = x + weights[j] * vs[j][...]
        r = r - weights[j] * ws[j][...]
    solution[...] = x
    residual[...] = r


def body(tiles, codes, counts, right_side, initial_guess):
    shape = Shape(codes)
    blk = tiles.shape[-1]
    flat = (shape.nb, blk)
    guess = initial_guess.reshape(flat)
    right = right_side.reshape(flat)
    vmem = pl.BlockSpec(memory_space=pltpu.VMEM)
    vector = jax.ShapeDtypeStruct(flat, jnp.float32)
    small = jax.ShapeDtypeStruct((1, blk), jnp.float32)
    buffer = jax.ShapeDtypeStruct((shape.nd, shape.rows, 1, blk), jnp.float32)
    halo = jax.ShapeDtypeStruct((shape.nd, shape.rows - 1, 1, blk), jnp.float32)
    params = pltpu.CompilerParams(vmem_limit_bytes=VMEM_BYTES)
    padded = pltpu.VMEM((shape.zero + 1, 1, blk), jnp.float32)

    def exchange(send):
        return lax.all_to_all(send, AXES, 0, 0, tiled=True)

    send = pl.pallas_call(
        functools.partial(first_kernel, shape),
        out_shape=halo,
        in_specs=[vmem] + [pl.BlockSpec(memory_space=pltpu.HBM)] * 4,
        out_specs=vmem,
        compiler_params=params,
        name="first",
    )(guess, *(pltpu.with_memory_space_constraint(x, pltpu.HBM) for x in (tiles, right, codes, counts)))
    recv = exchange(send)
    send, start, index = pl.pallas_call(
        functools.partial(start_kernel, shape),
        out_shape=(halo, vector, jax.ShapeDtypeStruct((shape.nb, shape.words), jnp.int32)),
        in_specs=[vmem] * 6,
        out_specs=(vmem,) * 3,
        scratch_shapes=[padded],
        compiler_params=params,
        name="start",
    )(codes, counts, tiles, recv, guess, right)
    recv = exchange(send)
    send, image = pl.pallas_call(
        functools.partial(first_step_kernel, shape),
        out_shape=(buffer, vector),
        in_specs=[vmem] * 4,
        out_specs=(vmem,) * 2,
        scratch_shapes=[padded],
        compiler_params=params,
        name="step0",
    )(index, tiles, recv, start)
    vs, ws, hs = [start], [image], []
    for step in range(1, ITERS):
        recv = exchange(send)
        final = step + 1 == ITERS
        out = buffer if not final else jax.ShapeDtypeStruct((shape.nd, 1, 1, blk), jnp.float32)
        more = (vector, vector, small) if step == 1 else ()
        send, v, w, h, *more = pl.pallas_call(
            functools.partial(step_kernel, shape, step),
            out_shape=(out, vector, vector, small, *more),
            in_specs=[vmem] * (3 + len(vs) + len(ws)),
            out_specs=(vmem,) * (4 + len(more)),
            scratch_shapes=[padded],
            compiler_params=params,
            name=f"step{step}",
        )(index, tiles, recv, *vs, *ws)
        if step == 1:
            v0, w0, beta = more
            vs, ws, hs = [v0], [w0], [beta]
        vs.append(v)
        ws.append(w)
        hs.append(h)
    recv = exchange(send)
    solution, residual, hessenberg = pl.pallas_call(
        functools.partial(last_kernel, shape),
        out_shape=(vector, vector, jax.ShapeDtypeStruct((ITERS, ITERS + 1), jnp.float32)),
        in_specs=[vmem] * (3 + 3 * ITERS),
        out_specs=(vmem,) * 3,
        compiler_params=params,
        name="last",
    )(recv, guess, start, *vs, *ws, *hs)
    whole = initial_guess.shape
    return solution.reshape(whole), residual.reshape(whole), hessenberg.T


def solution(mesh):
    placed = (
        P("gx", "gy", None, None, None),
        P("gx", "gy", None),
        P("gx", "gy"),
        P("gx", "gy", None),
        P("gx", "gy", None),
    )
    return jax.shard_map(
        body,
        mesh=mesh,
        in_specs=placed,
        out_specs=(P("gx", "gy", None), P("gx", "gy", None), P()),
        check_vma=False,
    )
```

```python
import functools

import jax
import jax.numpy as jnp
from jax import lax
from jax.experimental import pallas as pl
from jax.experimental.pallas import tpu as pltpu
from jax.sharding import PartitionSpec as P

ITERS = 4
AXES = ("gx", "gy")
VMEM_BYTES = 12 * 1024 * 1024
OFFSETS = [(dx, dy) for dx in (-1, 0, 1) for dy in (-1, 0, 1) if (dx, dy) != (0, 0)]


class Shape:
    def __init__(self, codes):
        self.rx, self.ry, self.slots = codes.shape
        self.nb = self.rx * self.ry
        self.nx = lax.axis_size("gx")
        self.ny = lax.axis_size("gy")
        self.nd = self.nx * self.ny
        self.rows = max(self.rx, self.ry) + 1
        self.width = self.ry + 2
        self.zero = (self.rx + 2) * (self.ry + 2)
        self.bits = self.zero.bit_length()
        self.fields = 31 // self.bits
        self.words = -(-self.slots // self.fields)

    def edge(self, dx, dy):
        xs = {-1: [0], 0: range(self.rx), 1: [self.rx - 1]}[dx]
        ys = {-1: [0], 0: range(self.ry), 1: [self.ry - 1]}[dy]
        return [(x, y) for x in xs for y in ys]

    def halo(self, dx, dy):
        xs = {-1: [0], 0: range(1, self.rx + 1), 1: [self.rx + 1]}[dx]
        ys = {-1: [0], 0: range(1, self.ry + 1), 1: [self.ry + 1]}[dy]
        return [x * self.width + y for x in xs for y in ys]


def neighbour(shape, dx, dy):
    ix, iy = lax.axis_index("gx"), lax.axis_index("gy")
    x, y = ix + dx, iy + dy
    inside = (x >= 0) & (x < shape.nx) & (y >= 0) & (y < shape.ny)
    return jnp.where(inside, x * shape.ny + y, ix * shape.ny + iy)


def pack(shape, rows, send):
    for dx, dy in OFFSETS:
        dst = neighbour(shape, dx, dy)
        for k, (x, y) in enumerate(shape.edge(dx, dy)):
            send[dst, k] = rows[x * shape.ry + y]


def unpack(shape, recv, own, padded):
    for x in range(shape.rx):
        for y in range(shape.ry):
            padded[(x + 1) * shape.width + y + 1] = own[x * shape.ry + y]
    for dx, dy in OFFSETS:
        src = neighbour(shape, dx, dy)
        for k, position in enumerate(shape.halo(dx, dy)):
            padded[position] = recv[src, k]
    padded[shape.zero] = jnp.zeros_like(padded[shape.zero])


def table(shape, codes, counts, index):
    size = (shape.ry, shape.slots)
    slot = lax.broadcasted_iota(jnp.int32, size, 1)
    square = (shape.ry, shape.ry)
    eye = lax.broadcasted_iota(jnp.int32, square, 0) == lax.broadcasted_iota(jnp.int32, square, 1)
    for x in range(shape.rx):
        code = codes[x]
        row = counts[x : x + 1, :].astype(jnp.float32)
        count = jnp.sum(jnp.where(eye, row, 0.0), axis=1, keepdims=True).astype(jnp.int32)
        down = jnp.where(code >= 6, 2, jnp.where(code >= 3, 1, 0))
        px = x + down
        py = lax.broadcasted_iota(jnp.int32, size, 0) + code - 3 * down
        gx = lax.axis_index("gx") * shape.rx + px - 1
        gy = lax.axis_index("gy") * shape.ry + py - 1
        live = slot < count
        live &= (gx >= 0) & (gx < shape.nx * shape.rx) & (gy >= 0) & (gy < shape.ny * shape.ry)
        place = jnp.where(live, px * shape.width + py, shape.zero)
        place = place << (lax.rem(slot, shape.fields) * shape.bits)
        for w in range(shape.words):
            word = None
            for s in range(w * shape.fields, min((w + 1) * shape.fields, shape.slots)):
                field = place[:, s : s + 1]
                word = field if word is None else word | field
            index[x * shape.ry : (x + 1) * shape.ry, w : w + 1] = word


def matvec(shape, index, tiles, padded):
    blk = tiles.shape[-1]
    eye = lax.broadcasted_iota(jnp.int32, (blk, blk), 0) == lax.broadcasted_iota(
        jnp.int32, (blk, blk), 1
    )
    out = []
    words = [[index[b : b + 1, w : w + 1][0, 0] for w in range(shape.words)] for b in range(shape.nb)]
    for b in range(shape.nb):
        x, y = divmod(b, shape.ry)
        total = None
        for s in range(shape.slots):
            word, place = divmod(s, shape.fields)
            row = (words[b][word] >> (place * shape.bits)) & ((1 << shape.bits) - 1)
            term = tiles[x, y, s] * padded[row]
            total = term if total is None else total + term
        column = jnp.sum(total, axis=1, keepdims=True)
        row = jnp.zeros((8, blk), jnp.float32)
        for k in range(0, blk, 8):
            row = jnp.where(eye[k : k + 8], column[k : k + 8], row)
        out.append(jnp.sum(row, axis=0, keepdims=True))
    return jnp.concatenate(out, axis=0)


def single(row, i):
    return row[:, i : i + 1]


def lane(row, i):
    return jnp.broadcast_to(row[:, i : i + 1], row.shape)


def inner(a, b):
    return jnp.sum(jnp.sum(a * b, axis=1, keepdims=True), axis=0, keepdims=True)


def spread(values):
    place = lax.broadcasted_iota(jnp.int32, (1, 128), 1)
    row = jnp.zeros((1, 128), jnp.float32)
    for i, value in enumerate(values):
        row = jnp.where(place == i, value, row)
    return row


def send_dots(shape, row, send):
    for d in range(shape.nd):
        send[d, shape.rows - 1] = row


def sum_dots(shape, recv, at, count, pick):
    parts = [recv[d, at] for d in range(shape.nd)]
    while len(parts) > 1:
        parts = [a + b for a, b in zip(parts[::2], parts[1::2])] + (
            [parts[-1]] if len(parts) % 2 else []
        )
    return [pick(parts[0], i) for i in range(count)]


def split(value):
    return [value[b : b + 1] for b in range(value.shape[0])]


def first_kernel(shape, guess, *refs):
    send = refs[-1]
    rows = [guess[b : b + 1, :] for b in range(shape.nb)]
    pack(shape, rows, send)


def start_kernel(shape, codes, counts, tiles, recv, guess, right, send, start, index, padded):
    table(shape, codes, counts, index)
    unpack(shape, recv, [guess[b : b + 1, :] for b in range(shape.nb)], padded)
    r = right[...] - matvec(shape, index, tiles, padded)
    start[...] = r
    pack(shape, split(r), send)


def first_step_kernel(shape, index, tiles, recv, start, send, image, padded):
    r = start[...]
    unpack(shape, recv, split(r), padded)
    t = matvec(shape, index, tiles, padded)
    image[...] = t
    pack(shape, split(t), send)
    send_dots(shape, spread([inner(r, r), inner(t, r), inner(t, t)]), send)


def step_kernel(shape, step, index, tiles, recv, *refs):
    count = 2 * step
    keep, outs = refs[:count], list(refs[count:])
    padded = outs.pop()
    last = keep[-1][...]
    unpack(shape, recv, split(last), padded)
    image = matvec(shape, index, tiles, padded)
    if step == 1:
        whole, cross, square = sum_dots(shape, recv, shape.rows - 1, 3, single)
        beta = jnp.sqrt(whole)
        inverse = 1.0 / beta
        sums = [cross / whole]
        square = square / whole
        basis = [keep[0][...] * inverse]
        images = [last * inverse]
        image = image * inverse
    else:
        *sums, square = sum_dots(shape, recv, shape.rows - 1, step + 1, single)
        basis = [ref[...] for ref in keep[:step]]
        images = [ref[...] for ref in keep[step:]]
    for value in sums:
        square = square - value * value
    length = jnp.sqrt(square)
    scale = 1.0 / length
    v, w = images[-1], image
    for value, b, a in zip(sums, basis, images):
        v = v - value * b
        w = w - value * a
    v = v * scale
    w = w * scale
    if step + 1 < ITERS:
        pack(shape, split(w), outs[0])
    row = spread([inner(w, other) for other in basis + [v, w]])
    if step + 1 < ITERS:
        send_dots(shape, row, outs[0])
    else:
        for d in range(shape.nd):
            outs[0][d, 0] = row
    outs[1][...] = v
    outs[2][...] = w
    outs[3][...] = spread(sums + [length])
    if step == 1:
        outs[4][...] = basis[0]
        outs[5][...] = images[0]
        outs[6][...] = spread([beta])


def last_kernel(shape, recv, guess, start, *refs):
    vs, ws, hs, (solution, residual, hess) = (
        refs[:ITERS],
        refs[ITERS : 2 * ITERS],
        refs[2 * ITERS : 3 * ITERS],
        refs[3 * ITERS :],
    )
    sums = sum_dots(shape, recv, 0, ITERS + 1, lane)
    square = sums[ITERS]
    for i in range(ITERS):
        square = square - sums[i] * sums[i]
    columns = []
    beta = lane(hs[0][...], 0)
    for j in range(1, ITERS):
        columns.append([lane(hs[j][...], i) for i in range(j + 1)])
    columns.append(sums[:ITERS] + [jnp.sqrt(square)])
    row = lax.broadcasted_iota(jnp.int32, hess.shape, 1)
    col = lax.broadcasted_iota(jnp.int32, hess.shape, 0)
    full = jnp.zeros(hess.shape, jnp.float32)
    for j, column in enumerate(columns):
        for i, value in enumerate(column):
            full = jnp.where((row == i) & (col == j), value[:, :1], full)
    hess[...] = full
    normal = {}
    for a in range(ITERS):
        for b in range(a + 1):
            total = None
            for p, q in zip(columns[a], columns[b]):
                total = p * q if total is None else total + p * q
            normal[a, b] = total
    lower, inverse = {}, {}
    for a in range(ITERS):
        for b in range(a + 1):
            total = normal[a, b]
            for c in range(b):
                total = total - lower[a, c] * lower[b, c]
            if a == b:
                inverse[a] = lax.rsqrt(total)
            else:
                lower[a, b] = total * inverse[b]
    forward = []
    for a in range(ITERS):
        total = beta * columns[a][0]
        for c in range(a):
            total = total - lower[a, c] * forward[c]
        forward.append(total * inverse[a])
    weights = [None] * ITERS
    for a in reversed(range(ITERS)):
        total = forward[a]
        for c in range(a + 1, ITERS):
            total = total - lower[c, a] * weights[c]
        weights[a] = total * inverse[a]
    x = guess[...]
    r = start[...]
    for j in range(ITERS):
        x = x + weights[j] * vs[j][...]
        r = r - weights[j] * ws[j][...]
    solution[...] = x
    residual[...] = r


def body(tiles, codes, counts, right_side, initial_guess):
    shape = Shape(codes)
    blk = tiles.shape[-1]
    flat = (shape.nb, blk)
    guess = initial_guess.reshape(flat)
    right = right_side.reshape(flat)
    vmem = pl.BlockSpec(memory_space=pltpu.VMEM)
    vector = jax.ShapeDtypeStruct(flat, jnp.float32)
    small = jax.ShapeDtypeStruct((1, blk), jnp.float32)
    buffer = jax.ShapeDtypeStruct((shape.nd, shape.rows, 1, blk), jnp.float32)
    halo = jax.ShapeDtypeStruct((shape.nd, shape.rows - 1, 1, blk), jnp.float32)
    params = pltpu.CompilerParams(vmem_limit_bytes=VMEM_BYTES)
    padded = pltpu.VMEM((shape.zero + 1, 1, blk), jnp.float32)

    def exchange(send):
        return lax.all_to_all(send, AXES, 0, 0, tiled=True)

    send = pl.pallas_call(
        functools.partial(first_kernel, shape),
        out_shape=halo,
        in_specs=[vmem] + [pl.BlockSpec(memory_space=pltpu.HBM)] * 4,
        out_specs=vmem,
        compiler_params=params,
        name="first",
    )(guess, *(pltpu.with_memory_space_constraint(x, pltpu.HBM) for x in (tiles, right, codes, counts)))
    recv = exchange(send)
    send, start, index = pl.pallas_call(
        functools.partial(start_kernel, shape),
        out_shape=(halo, vector, jax.ShapeDtypeStruct((shape.nb, shape.words), jnp.int32)),
        in_specs=[vmem] * 6,
        out_specs=(vmem,) * 3,
        scratch_shapes=[padded],
        compiler_params=params,
        name="start",
    )(codes, counts, tiles, recv, guess, right)
    recv = exchange(send)
    send, image = pl.pallas_call(
        functools.partial(first_step_kernel, shape),
        out_shape=(buffer, vector),
        in_specs=[vmem] * 4,
        out_specs=(vmem,) * 2,
        scratch_shapes=[padded],
        compiler_params=params,
        name="step0",
    )(index, tiles, recv, start)
    vs, ws, hs = [start], [image], []
    for step in range(1, ITERS):
        recv = exchange(send)
        final = step + 1 == ITERS
        out = buffer if not final else jax.ShapeDtypeStruct((shape.nd, 1, 1, blk), jnp.float32)
        more = (vector, vector, small) if step == 1 else ()
        send, v, w, h, *more = pl.pallas_call(
            functools.partial(step_kernel, shape, step),
            out_shape=(out, vector, vector, small, *more),
            in_specs=[vmem] * (3 + len(vs) + len(ws)),
            out_specs=(vmem,) * (4 + len(more)),
            scratch_shapes=[padded],
            compiler_params=params,
            name=f"step{step}",
        )(index, tiles, recv, *vs, *ws)
        if step == 1:
            v0, w0, beta = more
            vs, ws, hs = [v0], [w0], [beta]
        vs.append(v)
        ws.append(w)
        hs.append(h)
    recv = exchange(send)
    solution, residual, hessenberg = pl.pallas_call(
        functools.partial(last_kernel, shape),
        out_shape=(vector, vector, jax.ShapeDtypeStruct((ITERS, ITERS + 1), jnp.float32)),
        in_specs=[vmem] * (3 + 3 * ITERS),
        out_specs=(vmem,) * 3,
        compiler_params=params,
        name="last",
    )(recv, guess, start, *vs, *ws, *hs)
    whole = initial_guess.shape
    return solution.reshape(whole), residual.reshape(whole), hessenberg.T


def solution(mesh):
    placed = (
        P("gx", "gy", None, None, None),
        P("gx", "gy", None),
        P("gx", "gy"),
        P("gx", "gy", None),
        P("gx", "gy", None),
    )
    return jax.shard_map(
        body,
        mesh=mesh,
        in_specs=placed,
        out_specs=(P("gx", "gy", None), P("gx", "gy", None), P()),
        check_vma=False,
    )
```

```python
import functools

import jax
import jax.numpy as jnp
from jax import lax
from jax.experimental import pallas as pl
from jax.experimental.pallas import tpu as pltpu
from jax.sharding import PartitionSpec as P

ITERS = 4
SHIFT = 3.0
AXES = ("gx", "gy")
VMEM_BYTES = 12 * 1024 * 1024
OFFSETS = [(dx, dy) for dx in (-1, 0, 1) for dy in (-1, 0, 1) if (dx, dy) != (0, 0)]


class Shape:
    def __init__(self, codes):
        self.rx, self.ry, self.slots = codes.shape
        self.nb = self.rx * self.ry
        self.nx = lax.axis_size("gx")
        self.ny = lax.axis_size("gy")
        self.nd = self.nx * self.ny
        self.rows = max(self.rx, self.ry) + 1
        self.width = self.ry + 2
        self.zero = (self.rx + 2) * (self.ry + 2)
        self.bits = self.zero.bit_length()
        self.fields = 31 // self.bits
        self.words = -(-self.slots // self.fields)

    def edge(self, dx, dy):
        xs = {-1: [0], 0: range(self.rx), 1: [self.rx - 1]}[dx]
        ys = {-1: [0], 0: range(self.ry), 1: [self.ry - 1]}[dy]
        return [(x, y) for x in xs for y in ys]

    def halo(self, dx, dy):
        xs = {-1: [0], 0: range(1, self.rx + 1), 1: [self.rx + 1]}[dx]
        ys = {-1: [0], 0: range(1, self.ry + 1), 1: [self.ry + 1]}[dy]
        return [x * self.width + y for x in xs for y in ys]


def neighbour(shape, dx, dy):
    ix, iy = lax.axis_index("gx"), lax.axis_index("gy")
    x, y = ix + dx, iy + dy
    inside = (x >= 0) & (x < shape.nx) & (y >= 0) & (y < shape.ny)
    return jnp.where(inside, x * shape.ny + y, ix * shape.ny + iy)


def pack(shape, rows, send):
    for dx, dy in OFFSETS:
        dst = neighbour(shape, dx, dy)
        for k, (x, y) in enumerate(shape.edge(dx, dy)):
            send[dst, k] = rows[x * shape.ry + y]


def unpack(shape, recv, own, padded):
    for x in range(shape.rx):
        for y in range(shape.ry):
            padded[(x + 1) * shape.width + y + 1] = own[x * shape.ry + y]
    for dx, dy in OFFSETS:
        src = neighbour(shape, dx, dy)
        for k, position in enumerate(shape.halo(dx, dy)):
            padded[position] = recv[src, k]
    padded[shape.zero] = jnp.zeros_like(padded[shape.zero])


def table(shape, codes, counts, index):
    size = (shape.ry, shape.slots)
    slot = lax.broadcasted_iota(jnp.int32, size, 1)
    square = (shape.ry, shape.ry)
    eye = lax.broadcasted_iota(jnp.int32, square, 0) == lax.broadcasted_iota(jnp.int32, square, 1)
    for x in range(shape.rx):
        code = codes[x]
        row = counts[x : x + 1, :].astype(jnp.float32)
        count = jnp.sum(jnp.where(eye, row, 0.0), axis=1, keepdims=True).astype(jnp.int32)
        down = jnp.where(code >= 6, 2, jnp.where(code >= 3, 1, 0))
        px = x + down
        py = lax.broadcasted_iota(jnp.int32, size, 0) + code - 3 * down
        gx = lax.axis_index("gx") * shape.rx + px - 1
        gy = lax.axis_index("gy") * shape.ry + py - 1
        live = slot < count
        live &= (gx >= 0) & (gx < shape.nx * shape.rx) & (gy >= 0) & (gy < shape.ny * shape.ry)
        place = jnp.where(live, px * shape.width + py, shape.zero)
        place = place << (lax.rem(slot, shape.fields) * shape.bits)
        for w in range(shape.words):
            word = None
            for s in range(w * shape.fields, min((w + 1) * shape.fields, shape.slots)):
                field = place[:, s : s + 1]
                word = field if word is None else word | field
            index[x * shape.ry : (x + 1) * shape.ry, w : w + 1] = word


def matvec(shape, index, tiles, padded):
    blk = tiles.shape[-1]
    eye = lax.broadcasted_iota(jnp.int32, (blk, blk), 0) == lax.broadcasted_iota(
        jnp.int32, (blk, blk), 1
    )
    out = []
    words = [[index[b : b + 1, w : w + 1][0, 0] for w in range(shape.words)] for b in range(shape.nb)]
    for b in range(shape.nb):
        x, y = divmod(b, shape.ry)
        total = None
        for s in range(shape.slots):
            word, place = divmod(s, shape.fields)
            row = (words[b][word] >> (place * shape.bits)) & ((1 << shape.bits) - 1)
            term = tiles[x, y, s] * padded[row]
            total = term if total is None else total + term
        column = jnp.sum(total, axis=1, keepdims=True)
        row = jnp.zeros((8, blk), jnp.float32)
        for k in range(0, blk, 8):
            row = jnp.where(eye[k : k + 8], column[k : k + 8], row)
        out.append(jnp.sum(row, axis=0, keepdims=True))
    return jnp.concatenate(out, axis=0)


def single(row, i):
    return row[:, i : i + 1]


def lane(row, i):
    return jnp.broadcast_to(row[:, i : i + 1], row.shape)


def inner(a, b):
    return jnp.sum(jnp.sum(a * b, axis=1, keepdims=True), axis=0, keepdims=True)


def spread(values):
    place = lax.broadcasted_iota(jnp.int32, (1, 128), 1)
    row = jnp.zeros((1, 128), jnp.float32)
    for i, value in enumerate(values):
        row = jnp.where(place == i, value, row)
    return row


def send_dots(shape, row, send):
    for d in range(shape.nd):
        send[d, shape.rows - 1] = row


def sum_dots(shape, recv, at, count, pick):
    parts = [recv[d, at] for d in range(shape.nd)]
    while len(parts) > 1:
        parts = [a + b for a, b in zip(parts[::2], parts[1::2])] + (
            [parts[-1]] if len(parts) % 2 else []
        )
    return [pick(parts[0], i) for i in range(count)]


def split(value):
    return [value[b : b + 1] for b in range(value.shape[0])]


def first_kernel(shape, guess, *refs):
    send = refs[-1]
    rows = [guess[b : b + 1, :] for b in range(shape.nb)]
    pack(shape, rows, send)


def start_kernel(shape, codes, counts, tiles, recv, guess, right, send, start, index, padded):
    table(shape, codes, counts, index)
    unpack(shape, recv, [guess[b : b + 1, :] for b in range(shape.nb)], padded)
    r = right[...] - matvec(shape, index, tiles, padded)
    start[...] = r
    pack(shape, split(r), send)


def first_step_kernel(shape, index, tiles, recv, start, send, image, padded):
    r = start[...]
    unpack(shape, recv, split(r), padded)
    t = matvec(shape, index, tiles, padded)
    image[...] = t
    pack(shape, split(t), send)
    u = t - SHIFT * r
    send_dots(shape, spread([inner(r, r), inner(u, r), inner(u, u)]), send)


def step_kernel(shape, step, index, tiles, recv, *refs):
    count = 2 * step
    keep, outs = refs[:count], list(refs[count:])
    padded = outs.pop()
    last = keep[-1][...]
    unpack(shape, recv, split(last), padded)
    image = matvec(shape, index, tiles, padded)
    if step == 1:
        whole, cross, square = sum_dots(shape, recv, shape.rows - 1, 3, single)
        beta = jnp.sqrt(whole)
        inverse = 1.0 / beta
        sums = [cross / whole]
        square = square / whole
        basis = [keep[0][...] * inverse]
        images = [last * inverse]
        image = image * inverse
    else:
        *sums, square = sum_dots(shape, recv, shape.rows - 1, step + 1, single)
        basis = [ref[...] for ref in keep[:step]]
        images = [ref[...] for ref in keep[step:]]
    for value in sums:
        square = square - value * value
    sums[-1] = sums[-1] + SHIFT
    length = jnp.sqrt(square)
    scale = 1.0 / length
    v, w = images[-1], image
    for value, b, a in zip(sums, basis, images):
        v = v - value * b
        w = w - value * a
    v = v * scale
    w = w * scale
    if step + 1 < ITERS:
        pack(shape, split(w), outs[0])
    u = w - SHIFT * v
    row = spread([inner(u, other) for other in basis + [v, u]])
    if step + 1 < ITERS:
        send_dots(shape, row, outs[0])
    else:
        for d in range(shape.nd):
            outs[0][d, 0] = row
    outs[1][...] = v
    outs[2][...] = w
    outs[3][...] = spread(sums + [length])
    if step == 1:
        outs[4][...] = basis[0]
        outs[5][...] = images[0]
        outs[6][...] = spread([beta])


def last_kernel(shape, recv, guess, start, *refs):
    vs, ws, hs, (solution, residual, hess) = (
        refs[:ITERS],
        refs[ITERS : 2 * ITERS],
        refs[2 * ITERS : 3 * ITERS],
        refs[3 * ITERS :],
    )
    sums = sum_dots(shape, recv, 0, ITERS + 1, lane)
    square = sums[ITERS]
    for i in range(ITERS):
        square = square - sums[i] * sums[i]
    sums[ITERS - 1] = sums[ITERS - 1] + SHIFT
    columns = []
    beta = lane(hs[0][...], 0)
    for j in range(1, ITERS):
        columns.append([lane(hs[j][...], i) for i in range(j + 1)])
    columns.append(sums[:ITERS] + [jnp.sqrt(square)])
    row = lax.broadcasted_iota(jnp.int32, hess.shape, 1)
    col = lax.broadcasted_iota(jnp.int32, hess.shape, 0)
    full = jnp.zeros(hess.shape, jnp.float32)
    for j, column in enumerate(columns):
        for i, value in enumerate(column):
            full = jnp.where((row == i) & (col == j), value[:, :1], full)
    hess[...] = full
    normal = {}
    for a in range(ITERS):
        for b in range(a + 1):
            total = None
            for p, q in zip(columns[a], columns[b]):
                total = p * q if total is None else total + p * q
            normal[a, b] = total
    lower, inverse = {}, {}
    for a in range(ITERS):
        for b in range(a + 1):
            total = normal[a, b]
            for c in range(b):
                total = total - lower[a, c] * lower[b, c]
            if a == b:
                inverse[a] = lax.rsqrt(total)
            else:
                lower[a, b] = total * inverse[b]
    forward = []
    for a in range(ITERS):
        total = beta * columns[a][0]
        for c in range(a):
            total = total - lower[a, c] * forward[c]
        forward.append(total * inverse[a])
    weights = [None] * ITERS
    for a in reversed(range(ITERS)):
        total = forward[a]
        for c in range(a + 1, ITERS):
            total = total - lower[c, a] * weights[c]
        weights[a] = total * inverse[a]
    x = guess[...]
    r = start[...]
    for j in range(ITERS):
        x = x + weights[j] * vs[j][...]
        r = r - weights[j] * ws[j][...]
    solution[...] = x
    residual[...] = r


def body(tiles, codes, counts, right_side, initial_guess):
    shape = Shape(codes)
    blk = tiles.shape[-1]
    flat = (shape.nb, blk)
    guess = initial_guess.reshape(flat)
    right = right_side.reshape(flat)
    vmem = pl.BlockSpec(memory_space=pltpu.VMEM)
    vector = jax.ShapeDtypeStruct(flat, jnp.float32)
    small = jax.ShapeDtypeStruct((1, blk), jnp.float32)
    buffer = jax.ShapeDtypeStruct((shape.nd, shape.rows, 1, blk), jnp.float32)
    halo = jax.ShapeDtypeStruct((shape.nd, shape.rows - 1, 1, blk), jnp.float32)
    params = pltpu.CompilerParams(vmem_limit_bytes=VMEM_BYTES)
    padded = pltpu.VMEM((shape.zero + 1, 1, blk), jnp.float32)

    def exchange(send):
        return lax.all_to_all(send, AXES, 0, 0, tiled=True)

    send = pl.pallas_call(
        functools.partial(first_kernel, shape),
        out_shape=halo,
        in_specs=[vmem] + [pl.BlockSpec(memory_space=pltpu.HBM)] * 4,
        out_specs=vmem,
        compiler_params=params,
        name="first",
    )(guess, *(pltpu.with_memory_space_constraint(x, pltpu.HBM) for x in (tiles, right, codes, counts)))
    recv = exchange(send)
    send, start, index = pl.pallas_call(
        functools.partial(start_kernel, shape),
        out_shape=(halo, vector, jax.ShapeDtypeStruct((shape.nb, shape.words), jnp.int32)),
        in_specs=[vmem] * 6,
        out_specs=(vmem,) * 3,
        scratch_shapes=[padded],
        compiler_params=params,
        name="start",
    )(codes, counts, tiles, recv, guess, right)
    recv = exchange(send)
    send, image = pl.pallas_call(
        functools.partial(first_step_kernel, shape),
        out_shape=(buffer, vector),
        in_specs=[vmem] * 4,
        out_specs=(vmem,) * 2,
        scratch_shapes=[padded],
        compiler_params=params,
        name="step0",
    )(index, tiles, recv, start)
    vs, ws, hs = [start], [image], []
    for step in range(1, ITERS):
        recv = exchange(send)
        final = step + 1 == ITERS
        out = buffer if not final else jax.ShapeDtypeStruct((shape.nd, 1, 1, blk), jnp.float32)
        more = (vector, vector, small) if step == 1 else ()
        send, v, w, h, *more = pl.pallas_call(
            functools.partial(step_kernel, shape, step),
            out_shape=(out, vector, vector, small, *more),
            in_specs=[vmem] * (3 + len(vs) + len(ws)),
            out_specs=(vmem,) * (4 + len(more)),
            scratch_shapes=[padded],
            compiler_params=params,
            name=f"step{step}",
        )(index, tiles, recv, *vs, *ws)
        if step == 1:
            v0, w0, beta = more
            vs, ws, hs = [v0], [w0], [beta]
        vs.append(v)
        ws.append(w)
        hs.append(h)
    recv = exchange(send)
    solution, residual, hessenberg = pl.pallas_call(
        functools.partial(last_kernel, shape),
        out_shape=(vector, vector, jax.ShapeDtypeStruct((ITERS, ITERS + 1), jnp.float32)),
        in_specs=[vmem] * (3 + 3 * ITERS),
        out_specs=(vmem,) * 3,
        compiler_params=params,
        name="last",
    )(recv, guess, start, *vs, *ws, *hs)
    whole = initial_guess.shape
    return solution.reshape(whole), residual.reshape(whole), hessenberg.T


def solution(mesh):
    placed = (
        P("gx", "gy", None, None, None),
        P("gx", "gy", None),
        P("gx", "gy"),
        P("gx", "gy", None),
        P("gx", "gy", None),
    )
    return jax.shard_map(
        body,
        mesh=mesh,
        in_specs=placed,
        out_specs=(P("gx", "gy", None), P("gx", "gy", None), P()),
        check_vma=False,
    )
```

```python
import functools

import jax
import jax.numpy as jnp
from jax import lax
from jax.experimental import pallas as pl
from jax.experimental.pallas import tpu as pltpu
from jax.sharding import PartitionSpec as P

ITERS = 4
SHIFT = 3.0
AXES = ("gx", "gy")
VMEM_BYTES = 12 * 1024 * 1024
OFFSETS = [(dx, dy) for dx in (-1, 0, 1) for dy in (-1, 0, 1) if (dx, dy) != (0, 0)]


class Shape:
    def __init__(self, codes):
        self.rx, self.ry, self.slots = codes.shape
        self.nb = self.rx * self.ry
        self.nx = lax.axis_size("gx")
        self.ny = lax.axis_size("gy")
        self.nd = self.nx * self.ny
        self.rows = max(self.rx, self.ry) + 1
        self.width = self.ry + 2
        self.zero = (self.rx + 2) * (self.ry + 2)
        self.bits = self.zero.bit_length()
        self.fields = 31 // self.bits
        self.words = -(-self.slots // self.fields)

    def edge(self, dx, dy):
        xs = {-1: [0], 0: range(self.rx), 1: [self.rx - 1]}[dx]
        ys = {-1: [0], 0: range(self.ry), 1: [self.ry - 1]}[dy]
        return [(x, y) for x in xs for y in ys]

    def halo(self, dx, dy):
        xs = {-1: [0], 0: range(1, self.rx + 1), 1: [self.rx + 1]}[dx]
        ys = {-1: [0], 0: range(1, self.ry + 1), 1: [self.ry + 1]}[dy]
        return [x * self.width + y for x in xs for y in ys]


def neighbour(shape, dx, dy):
    ix, iy = lax.axis_index("gx"), lax.axis_index("gy")
    x, y = ix + dx, iy + dy
    inside = (x >= 0) & (x < shape.nx) & (y >= 0) & (y < shape.ny)
    return jnp.where(inside, x * shape.ny + y, ix * shape.ny + iy)


def pack(shape, rows, send):
    for dx, dy in OFFSETS:
        dst = neighbour(shape, dx, dy)
        for k, (x, y) in enumerate(shape.edge(dx, dy)):
            send[dst, k] = rows[x * shape.ry + y]


def unpack(shape, recv, own, padded):
    for x in range(shape.rx):
        for y in range(shape.ry):
            padded[(x + 1) * shape.width + y + 1] = own[x * shape.ry + y]
    for dx, dy in OFFSETS:
        src = neighbour(shape, dx, dy)
        for k, position in enumerate(shape.halo(dx, dy)):
            padded[position] = recv[src, k]
    padded[shape.zero] = jnp.zeros_like(padded[shape.zero])


def table(shape, codes, counts, index):
    size = (shape.ry, shape.slots)
    slot = lax.broadcasted_iota(jnp.int32, size, 1)
    square = (shape.ry, shape.ry)
    eye = lax.broadcasted_iota(jnp.int32, square, 0) == lax.broadcasted_iota(jnp.int32, square, 1)
    for x in range(shape.rx):
        code = codes[x]
        row = counts[x : x + 1, :].astype(jnp.float32)
        count = jnp.sum(jnp.where(eye, row, 0.0), axis=1, keepdims=True).astype(jnp.int32)
        down = jnp.where(code >= 6, 2, jnp.where(code >= 3, 1, 0))
        px = x + down
        py = lax.broadcasted_iota(jnp.int32, size, 0) + code - 3 * down
        gx = lax.axis_index("gx") * shape.rx + px - 1
        gy = lax.axis_index("gy") * shape.ry + py - 1
        live = slot < count
        live &= (gx >= 0) & (gx < shape.nx * shape.rx) & (gy >= 0) & (gy < shape.ny * shape.ry)
        place = jnp.where(live, px * shape.width + py, shape.zero)
        place = place << (lax.rem(slot, shape.fields) * shape.bits)
        for w in range(shape.words):
            word = None
            for s in range(w * shape.fields, min((w + 1) * shape.fields, shape.slots)):
                field = place[:, s : s + 1]
                word = field if word is None else word | field
            index[x * shape.ry : (x + 1) * shape.ry, w : w + 1] = word


def matvec(shape, index, tiles, padded):
    blk = tiles.shape[-1]
    eye = lax.broadcasted_iota(jnp.int32, (blk, blk), 0) == lax.broadcasted_iota(
        jnp.int32, (blk, blk), 1
    )
    out = []
    words = [[index[b : b + 1, w : w + 1][0, 0] for w in range(shape.words)] for b in range(shape.nb)]
    for b in range(shape.nb):
        x, y = divmod(b, shape.ry)
        total = None
        for s in range(shape.slots):
            word, place = divmod(s, shape.fields)
            row = (words[b][word] >> (place * shape.bits)) & ((1 << shape.bits) - 1)
            term = tiles[x, y, s] * padded[row]
            total = term if total is None else total + term
        column = jnp.sum(total, axis=1, keepdims=True)
        halves = [jnp.zeros((8, blk), jnp.float32)] * 2
        for k in range(0, blk, 8):
            half = (k // 8) % 2
            halves[half] = jnp.where(eye[k : k + 8], column[k : k + 8], halves[half])
        out.append(jnp.sum(halves[0] + halves[1], axis=0, keepdims=True))
    return jnp.concatenate(out, axis=0)


def single(row, i):
    return row[:, i : i + 1]


def lane(row, i):
    return jnp.broadcast_to(row[:, i : i + 1], row.shape)


def inner(a, b):
    return jnp.sum(jnp.sum(a * b, axis=1, keepdims=True), axis=0, keepdims=True)


def spread(values):
    place = lax.broadcasted_iota(jnp.int32, (1, 128), 1)
    row = jnp.zeros((1, 128), jnp.float32)
    for i, value in enumerate(values):
        row = jnp.where(place == i, value, row)
    return row


def send_dots(shape, row, send):
    for d in range(shape.nd):
        send[d, shape.rows - 1] = row


def sum_dots(shape, recv, at, count, pick):
    parts = [recv[d, at] for d in range(shape.nd)]
    while len(parts) > 1:
        parts = [a + b for a, b in zip(parts[::2], parts[1::2])] + (
            [parts[-1]] if len(parts) % 2 else []
        )
    return [pick(parts[0], i) for i in range(count)]


def split(value):
    return [value[b : b + 1] for b in range(value.shape[0])]


def first_kernel(shape, guess, *refs):
    send = refs[-1]
    rows = [guess[b : b + 1, :] for b in range(shape.nb)]
    pack(shape, rows, send)


def start_kernel(shape, codes, counts, tiles, recv, guess, right, send, start, index, padded):
    table(shape, codes, counts, index)
    unpack(shape, recv, [guess[b : b + 1, :] for b in range(shape.nb)], padded)
    r = right[...] - matvec(shape, index, tiles, padded)
    start[...] = r
    pack(shape, split(r), send)


def first_step_kernel(shape, index, tiles, recv, start, send, image, padded):
    r = start[...]
    unpack(shape, recv, split(r), padded)
    t = matvec(shape, index, tiles, padded)
    image[...] = t
    pack(shape, split(t), send)
    u = t - SHIFT * r
    send_dots(shape, spread([inner(r, r), inner(u, r), inner(u, u)]), send)


def step_kernel(shape, step, index, tiles, recv, *refs):
    count = 2 * step
    keep, outs = refs[:count], list(refs[count:])
    padded = outs.pop()
    last = keep[-1][...]
    unpack(shape, recv, split(last), padded)
    image = matvec(shape, index, tiles, padded)
    if step == 1:
        whole, cross, square = sum_dots(shape, recv, shape.rows - 1, 3, single)
        beta = jnp.sqrt(whole)
        inverse = 1.0 / beta
        sums = [cross / whole]
        square = square / whole
        basis = [keep[0][...] * inverse]
        images = [last * inverse]
        image = image * inverse
    else:
        *sums, square = sum_dots(shape, recv, shape.rows - 1, step + 1, single)
        basis = [ref[...] for ref in keep[:step]]
        images = [ref[...] for ref in keep[step:]]
    for value in sums:
        square = square - value * value
    sums[-1] = sums[-1] + SHIFT
    length = jnp.sqrt(square)
    scale = 1.0 / length
    v, w = images[-1], image
    for value, b, a in zip(sums, basis, images):
        v = v - value * b
        w = w - value * a
    v = v * scale
    w = w * scale
    if step + 1 < ITERS:
        pack(shape, split(w), outs[0])
    u = w - SHIFT * v
    row = spread([inner(u, other) for other in basis + [v, u]])
    if step + 1 < ITERS:
        send_dots(shape, row, outs[0])
    else:
        for d in range(shape.nd):
            outs[0][d, 0] = row
    outs[1][...] = v
    outs[2][...] = w
    outs[3][...] = spread(sums + [length])
    if step == 1:
        outs[4][...] = basis[0]
        outs[5][...] = images[0]
        outs[6][...] = spread([beta])


def last_kernel(shape, recv, guess, start, *refs):
    vs, ws, hs, (solution, residual, hess) = (
        refs[:ITERS],
        refs[ITERS : 2 * ITERS],
        refs[2 * ITERS : 3 * ITERS],
        refs[3 * ITERS :],
    )
    sums = sum_dots(shape, recv, 0, ITERS + 1, lane)
    square = sums[ITERS]
    for i in range(ITERS):
        square = square - sums[i] * sums[i]
    sums[ITERS - 1] = sums[ITERS - 1] + SHIFT
    columns = []
    beta = lane(hs[0][...], 0)
    for j in range(1, ITERS):
        columns.append([lane(hs[j][...], i) for i in range(j + 1)])
    columns.append(sums[:ITERS] + [jnp.sqrt(square)])
    row = lax.broadcasted_iota(jnp.int32, hess.shape, 1)
    col = lax.broadcasted_iota(jnp.int32, hess.shape, 0)
    full = jnp.zeros(hess.shape, jnp.float32)
    for j, column in enumerate(columns):
        for i, value in enumerate(column):
            full = jnp.where((row == i) & (col == j), value[:, :1], full)
    hess[...] = full
    normal = {}
    for a in range(ITERS):
        for b in range(a + 1):
            total = None
            for p, q in zip(columns[a], columns[b]):
                total = p * q if total is None else total + p * q
            normal[a, b] = total
    lower, inverse = {}, {}
    for a in range(ITERS):
        for b in range(a + 1):
            total = normal[a, b]
            for c in range(b):
                total = total - lower[a, c] * lower[b, c]
            if a == b:
                inverse[a] = lax.rsqrt(total)
            else:
                lower[a, b] = total * inverse[b]
    forward = []
    for a in range(ITERS):
        total = beta * columns[a][0]
        for c in range(a):
            total = total - lower[a, c] * forward[c]
        forward.append(total * inverse[a])
    weights = [None] * ITERS
    for a in reversed(range(ITERS)):
        total = forward[a]
        for c in range(a + 1, ITERS):
            total = total - lower[c, a] * weights[c]
        weights[a] = total * inverse[a]
    x = guess[...]
    r = start[...]
    for j in range(ITERS):
        x = x + weights[j] * vs[j][...]
        r = r - weights[j] * ws[j][...]
    solution[...] = x
    residual[...] = r


def body(tiles, codes, counts, right_side, initial_guess):
    shape = Shape(codes)
    blk = tiles.shape[-1]
    flat = (shape.nb, blk)
    guess = initial_guess.reshape(flat)
    right = right_side.reshape(flat)
    vmem = pl.BlockSpec(memory_space=pltpu.VMEM)
    vector = jax.ShapeDtypeStruct(flat, jnp.float32)
    small = jax.ShapeDtypeStruct((1, blk), jnp.float32)
    buffer = jax.ShapeDtypeStruct((shape.nd, shape.rows, 1, blk), jnp.float32)
    halo = jax.ShapeDtypeStruct((shape.nd, shape.rows - 1, 1, blk), jnp.float32)
    params = pltpu.CompilerParams(vmem_limit_bytes=VMEM_BYTES)
    padded = pltpu.VMEM((shape.zero + 1, 1, blk), jnp.float32)

    def exchange(send):
        return lax.all_to_all(send, AXES, 0, 0, tiled=True)

    send = pl.pallas_call(
        functools.partial(first_kernel, shape),
        out_shape=halo,
        in_specs=[vmem] + [pl.BlockSpec(memory_space=pltpu.HBM)] * 4,
        out_specs=vmem,
        compiler_params=params,
        name="first",
    )(guess, *(pltpu.with_memory_space_constraint(x, pltpu.HBM) for x in (tiles, right, codes, counts)))
    recv = exchange(send)
    send, start, index = pl.pallas_call(
        functools.partial(start_kernel, shape),
        out_shape=(halo, vector, jax.ShapeDtypeStruct((shape.nb, shape.words), jnp.int32)),
        in_specs=[vmem] * 6,
        out_specs=(vmem,) * 3,
        scratch_shapes=[padded],
        compiler_params=params,
        name="start",
    )(codes, counts, tiles, recv, guess, right)
    recv = exchange(send)
    send, image = pl.pallas_call(
        functools.partial(first_step_kernel, shape),
        out_shape=(buffer, vector),
        in_specs=[vmem] * 4,
        out_specs=(vmem,) * 2,
        scratch_shapes=[padded],
        compiler_params=params,
        name="step0",
    )(index, tiles, recv, start)
    vs, ws, hs = [start], [image], []
    for step in range(1, ITERS):
        recv = exchange(send)
        final = step + 1 == ITERS
        out = buffer if not final else jax.ShapeDtypeStruct((shape.nd, 1, 1, blk), jnp.float32)
        more = (vector, vector, small) if step == 1 else ()
        send, v, w, h, *more = pl.pallas_call(
            functools.partial(step_kernel, shape, step),
            out_shape=(out, vector, vector, small, *more),
            in_specs=[vmem] * (3 + len(vs) + len(ws)),
            out_specs=(vmem,) * (4 + len(more)),
            scratch_shapes=[padded],
            compiler_params=params,
            name=f"step{step}",
        )(index, tiles, recv, *vs, *ws)
        if step == 1:
            v0, w0, beta = more
            vs, ws, hs = [v0], [w0], [beta]
        vs.append(v)
        ws.append(w)
        hs.append(h)
    recv = exchange(send)
    solution, residual, hessenberg = pl.pallas_call(
        functools.partial(last_kernel, shape),
        out_shape=(vector, vector, jax.ShapeDtypeStruct((ITERS, ITERS + 1), jnp.float32)),
        in_specs=[vmem] * (3 + 3 * ITERS),
        out_specs=(vmem,) * 3,
        compiler_params=params,
        name="last",
    )(recv, guess, start, *vs, *ws, *hs)
    whole = initial_guess.shape
    return solution.reshape(whole), residual.reshape(whole), hessenberg.T


def solution(mesh):
    placed = (
        P("gx", "gy", None, None, None),
        P("gx", "gy", None),
        P("gx", "gy"),
        P("gx", "gy", None),
        P("gx", "gy", None),
    )
    return jax.shard_map(
        body,
        mesh=mesh,
        in_specs=placed,
        out_specs=(P("gx", "gy", None), P("gx", "gy", None), P()),
        check_vma=False,
    )
```
